128 devices in a mesh: row: 8 (over z, x_lo), col: 16 (over y, x_hi, core).
Axes of the slice: x: 4 (x_hi: 2, x_lo: 2; x = x_hi * 2 + x_lo), y: 4, z: 4, core: 2. Of those that a mesh axis runs over, the one named last changes fastest.
Arguments:
- tokens: bfloat16 [256, 16384], P('row', 'col'), may hold values from -6 to 6
- probe_words: int32 [256, 512], P(None, 'col'), may hold values from -2147483648 to 2147483646, as said below
- token_ids: int32 [256], replicated, may hold values from 0 to 128255
- loss_weight: float32 [128256], replicated, may hold values from 0.5 to 2
- gate_weight: bfloat16 [16384, 26624], P('col', 'row'), may hold values from -0.046875 to 0.046875
- up_weight: bfloat16 [16384, 26624], P('col', 'row'), may hold values from -0.046875 to 0.046875
- down_weight: bfloat16 [26624, 16384], P('row', 'col'), may hold values from -0.0390625 to 0.0390625
Outputs:
- hvp: float32 [256, 16384], P('row', 'col')
The draws below stay inside these ranges and needn't reach their ends.
Inputs may be any that keep to these rules, and one draw needn't show every extreme that they name: `probe_words`: every bit of every word is an independent fair sign bit; bit k of word j of token t is the probe sign of feature 32 j + k of that token (set: +1, clear: -1).
All inputs are finite; a program needn't handle non-finite values.
Results may differ from the reference program's by a relative error of at most 0.0036.
Values may be sent and summed in bfloat16 or wider, within the bound.
A program may use at most 128 MiB of HBM per device.

```python
import math
import jax
import jax.numpy as jnp
import numpy as np
from jax import lax

D = 16384
FF = 26624
VOCAB = 128256
TOKENS = 256


def draw_probe_words(key, part):
    return jax.random.randint(key, (TOKENS, D // 32), -2147483648, 2147483647, dtype=jnp.int32)


def touch_ends(values, stream_key, smallest, top_value):
    place = [jax.random.randint(jax.random.fold_in(stream_key, axis), (), 0, length) for axis, length in enumerate(values.shape)]
    widest = values.shape.index(max(values.shape))
    neighbour = place[:widest] + [(place[widest] + 1) % values.shape[widest]] + place[widest + 1:]
    return values.at[tuple(place)].set(smallest).at[tuple(neighbour)].set(top_value)


def level_of(stream_key, extent, split, least, high):
    factor_of, own = 1.0, jax.random.fold_in(stream_key, 6)
    for position, parts in split:
        draws = jnp.exp(jax.random.uniform(jax.random.fold_in(own, position), (parts,), jnp.float32, least / len(split), high / len(split)))
        factor_of = factor_of * jnp.repeat(draws, extent[position] // parts).reshape([-1 if axis == position else 1 for axis in range(len(extent))])
    return factor_of


def ranked_wide(key, extent, count, lean):
    weights = [min(1 << octave, count + 1 - (1 << octave)) * (1 << 20) // math.isqrt((1 << octave) ** lean) + 1 for octave in range((count + 1).bit_length()) if 1 << octave <= count]
    scale = 1 + sum(weights) // (1 << 30)
    table = np.cumsum(np.array([max(1, weight // scale) for weight in weights]))
    pick = jax.random.randint(jax.random.fold_in(key, 1), extent, 0, int(table[len(weights) - 1]))
    start = jnp.left_shift(1, jnp.searchsorted(jnp.asarray(table, jnp.int32), pick, side="right").astype(jnp.int32))
    rank = start - 1 + jax.random.randint(jax.random.fold_in(key, 4), extent, 0, 1 << 30) % jnp.minimum(start, count + 1 - start)
    return jax.random.permutation(jax.random.fold_in(key, 2), count)[rank].astype(jnp.int32)


def gaussian(stream_key, shape, width, limit, cuts=(), kind=jnp.bfloat16):
    result = jax.random.normal(stream_key, shape, jnp.float32) * width
    if len(cuts) > 0:
        result = level_of(stream_key, shape, cuts, -0.22, 0.18) * result
    return jnp.clip(result, min=-limit, max=limit).astype(kind)


def setup_inputs(seed: int = 0) -> dict:
    key_of = jax.random.split(jax.random.key(seed), 8)
    tokens = gaussian(key_of[0], (TOKENS, D), 1.0, 6.0, ((0, 8), (1, 16)))
    probe_words = draw_probe_words(jax.random.fold_in(key_of[7], 71), 0)
    token_ids = touch_ends(ranked_wide(key_of[2], (TOKENS,), VOCAB, 2), jax.random.fold_in(key_of[2], 3), 0, VOCAB - 1).astype(jnp.int32)
    loss_weight = jnp.clip(jnp.exp(jax.random.uniform(key_of[3], (VOCAB,), jnp.float32, math.log(0.5), math.log(2.0))), 0.5, 2.0)
    gate_weight = gaussian(key_of[4], (D, FF), D ** -0.5, 0.046875, ((0, 16), (1, 8)))
    up_weight = gaussian(key_of[5], (D, FF), D ** -0.5, 0.046875, ((0, 16), (1, 8)))
    down_weight = gaussian(key_of[6], (FF, D), FF ** -0.5, 0.0390625, ((0, 8), (1, 16)))
    return dict(tokens=tokens, probe_words=probe_words, token_ids=token_ids, loss_weight=loss_weight, gate_weight=gate_weight, up_weight=up_weight, down_weight=down_weight)


def unpack_signs(packed):
    shifts = jnp.arange(32, dtype=jnp.int32)
    bit_vals = jnp.bitwise_and(jnp.right_shift(packed[:, :, None], shifts), 1)
    return (2 * bit_vals - 1).reshape(packed.shape[0], -1).astype(jnp.bfloat16)


def silu_parts(pre_act):
    sigmoid_pre = jax.nn.sigmoid(pre_act)
    active = pre_act * sigmoid_pre
    slopes = sigmoid_pre * (1.0 + pre_act * (1.0 - sigmoid_pre))
    curves = sigmoid_pre * (1.0 - sigmoid_pre) * (2.0 + pre_act * (1.0 - 2.0 * sigmoid_pre))
    return active, slopes, curves


def matmul(left_rows, weight):
    return jnp.dot(left_rows, weight, preferred_element_type=jnp.float32)


def matmul_trans(left_rows, weight):
    return lax.dot_general(left_rows, weight, (((1,), (1,)), ((), ())), preferred_element_type=jnp.float32)


def reference(tokens, probe_words, token_ids, loss_weight, gate_weight, up_weight, down_weight):
    probe = unpack_signs(probe_words)
    gate_pre = matmul(tokens, gate_weight)
    up_pre = matmul(tokens, up_weight)
    gate_tan = matmul(probe, gate_weight)
    up_tan = matmul(probe, up_weight)
    active, slopes, curves = silu_parts(gate_pre)
    hidden = (active * up_pre).astype(jnp.bfloat16)
    hidden_tan = (slopes * gate_tan * up_pre + active * up_tan).astype(jnp.bfloat16)
    output = matmul(hidden, down_weight)
    out_tan = matmul(hidden_tan, down_weight)
    weight_tok = jnp.take(loss_weight, token_ids)[:, None]
    cotangent = (weight_tok * (tokens.astype(jnp.float32) + output)).astype(jnp.bfloat16)
    cot_tan = weight_tok * (probe.astype(jnp.float32) + out_tan)
    cot_half = cot_tan.astype(jnp.bfloat16)
    backward = matmul_trans(cotangent, down_weight)
    back_tan = matmul_trans(cot_half, down_weight)
    gate_back = (back_tan * up_pre * slopes + backward * up_tan * slopes + backward * up_pre * curves * gate_tan).astype(jnp.bfloat16)
    up_back = (back_tan * active + backward * slopes * gate_tan).astype(jnp.bfloat16)
    return cot_tan + matmul_trans(gate_back, gate_weight) + matmul_trans(up_back, up_weight)
```

```python
import functools
import math

import jax
import jax.numpy as jnp
from jax import lax
from jax.experimental import pallas as pl
from jax.experimental.pallas import tpu as pltpu
from jax.sharding import PartitionSpec as P

MESH = pl.DeviceIdType.MESH
F32, BF16, I16, I32 = jnp.float32, jnp.bfloat16, jnp.int16, jnp.int32

TOK = 256
KD = 1024
HW = 3328
CW = 256
NJ = HW // CW
NF = KD // CW
LAG = (0, 2, 5, 8, 11, 14, 17, 20, 22)
SLOTS = 10

CODE_UNIT = 1024.0
CODE_SCALE = 32700.0 / math.log1p(4700.0 * CODE_UNIT)


def log_encode(x):
    mag = jnp.log(1.0 + jnp.abs(x) * CODE_UNIT) * CODE_SCALE
    q = (mag + 0.5).astype(I32)
    return jnp.where(x < 0, -q, q).astype(I16)


def log_decode(y):
    y = y.astype(I32).astype(F32)
    mag = (jnp.exp(jnp.abs(y) * (1.0 / CODE_SCALE)) - 1.0) * (1.0 / CODE_UNIT)
    return jnp.where(y < 0, -mag, mag)


def bf_encode(x):
    return x.astype(BF16)


def bf_decode(x):
    return x.astype(F32)


def dot(a, b):
    return jnp.dot(a, b, preferred_element_type=F32)


def dot_t(a, b):
    return lax.dot_general(a, b, (((1,), (1,)), ((), ())), preferred_element_type=F32)


def silu_parts(pre_act):
    sig = 1.0 / (1.0 + jnp.exp(-pre_act))
    active = pre_act * sig
    slopes = sig * (1.0 + pre_act * (1.0 - sig))
    curves = sig * (1.0 - sig) * (2.0 + pre_act * (1.0 - 2.0 * sig))
    return active, slopes, curves


def rdma(src, dst, ssem, rsem, dev):
    return pltpu.make_async_remote_copy(
        src_ref=src, dst_ref=dst, send_sem=ssem, recv_sem=rsem, device_id=dev, device_id_type=MESH
    )


class Ring:
    def __init__(self, pos, plus, minus, mate, side, rows, code, bufs, sems, x_code):
        self.pos, self.plus, self.minus, self.mate, self.side = pos, plus, minus, mate, side
        self.rows, self.half = rows, rows // 2
        self.enc, self.dec = code
        self.x_enc, self.x_dec = x_code
        self.opp_s, self.opp_r, self.nb_s, self.nb_r, self.x_s, self.x_r, self.keep = bufs
        self.ss, self.rs = sems

    def block(self, delta):
        return pl.multiple_of(lax.rem(self.pos + (4 + delta), 4) * self.rows, self.rows)

    def opp_copy(self, k, p):
        dev = self.plus if p == 0 else self.minus
        sl = lax.rem(k, SLOTS)
        return rdma(self.opp_s.at[sl, p], self.opp_r.at[k, p], self.ss.at[k, p], self.rs.at[k, p], dev)

    def nb_copy(self, k, d):
        dev = self.plus if d == 0 else self.minus
        sl = lax.rem(k, SLOTS)
        return rdma(self.nb_s.at[sl, d], self.nb_r.at[k, d], self.ss.at[k, 2 + d], self.rs.at[k, 2 + d], dev)

    def x_copy(self, k):
        sl = lax.rem(k, SLOTS)
        return rdma(self.x_s.at[sl], self.x_r.at[k], self.ss.at[k, 4], self.rs.at[k, 4], self.mate)

    def scatter(self, k, term):
        sl = lax.rem(k, SLOTS)
        for p in range(2):
            self.opp_s[sl, p] = self.enc(term(self.block(2), p))
        for p in range(2):
            self.opp_copy(k, p).start()
        self.keep[sl, 0] = term(self.block(1), 0)
        self.nb_s[sl, 0, 1] = self.enc(term(self.block(1), 1))
        self.nb_s[sl, 1, 0] = self.enc(term(self.block(-1), 0))
        self.keep[sl, 1] = term(self.block(-1), 1)
        for p in range(2):
            self.keep[sl, 2 + p] = term(self.block(0), p)

    def relay(self, k):
        sl = lax.rem(k, SLOTS)
        for p in range(2):
            self.opp_copy(k, p).wait()
            self.nb_s[sl, p, p] = self.enc(self.keep[sl, p] + self.dec(self.opp_r[k, p]))
            self.nb_copy(k, p).start()

    def gather_in(self, k):
        sl = lax.rem(k, SLOTS)
        for d in range(2):
            self.nb_copy(k, d).wait()
        other = pl.multiple_of((1 - self.side) * self.half, self.half)
        for p in range(2):
            self.keep[sl, 2 + p] += self.dec(self.nb_r[k, 0, p]) + self.dec(self.nb_r[k, 1, p])
            self.x_s[sl, p] = self.x_enc(self.keep[sl, 2 + p, pl.ds(other, self.half), :])
        self.x_copy(k).start()

    def finish(self, k):
        sl = lax.rem(k, SLOTS)
        self.x_copy(k).wait()
        own = pl.multiple_of(self.side * self.half, self.half)
        return [
            self.keep[sl, 2 + p, pl.ds(own, self.half), :] + self.x_dec(self.x_r[k, p]) for p in range(2)
        ]


class Spread:
    def __init__(self, pos, plus, minus, mate, side, rows, base, region, sems):
        self.pos, self.plus, self.minus, self.mate, self.side = pos, plus, minus, mate, side
        self.rows, self.half, self.base, self.region = rows, rows // 2, base, region
        self.ss, self.rs = sems

    def start_of(self, delta):
        return pl.multiple_of(self.base + lax.rem(self.pos + (4 + delta), 4) * self.rows, self.rows)

    def copy(self, k, i, ref, dev):
        return rdma(ref, ref, self.ss.at[k, i], self.rs.at[k, i], dev)

    def mine(self, k):
        at = pl.multiple_of(self.start_of(0) + self.side * self.half, self.half)
        return self.copy(k, 0, self.region(k, at, self.half, None), self.mate)

    def first(self, k):
        self.mine(k).start()

    def second(self, k):
        self.mine(k).wait_send()
        at = pl.multiple_of(self.start_of(0) + (1 - self.side) * self.half, self.half)
        self.copy(k, 0, self.region(k, at, self.half, None), self.mate).wait_recv()
        ref = self.region(k, self.start_of(0), self.rows, None)
        self.copy(k, 1, ref, self.plus).start()
        self.copy(k, 2, ref, self.minus).start()

    def third(self, k):
        ref = self.region(k, self.start_of(0), self.rows, None)
        self.copy(k, 1, ref, self.plus).wait_send()
        self.copy(k, 2, ref, self.minus).wait_send()
        self.copy(k, 1, self.region(k, self.start_of(-1), self.rows, None), self.plus).wait_recv()
        self.copy(k, 3, self.region(k, self.start_of(-1), self.rows, 0), self.plus).start()
        self.copy(k, 2, self.region(k, self.start_of(1), self.rows, None), self.minus).wait_recv()
        self.copy(k, 4, self.region(k, self.start_of(1), self.rows, 1), self.minus).start()

    def last(self, k):
        self.copy(k, 3, self.region(k, self.start_of(-1), self.rows, 0), self.plus).wait_send()
        self.copy(k, 4, self.region(k, self.start_of(1), self.rows, 1), self.minus).wait_send()
        self.copy(k, 3, self.region(k, self.start_of(2), self.rows, 0), self.plus).wait_recv()
        self.copy(k, 4, self.region(k, self.start_of(2), self.rows, 1), self.minus).wait_recv()


def block_kernel(
    tok_ref,
    words_ref,
    wt_ref,
    gate_hbm,
    up_hbm,
    down_hbm,
    out_ref,
    wg,
    wu,
    wd,
    lhs,
    cot,
    hid,
    back,
    res,
    d2d,
    keep,
    opp_s,
    opp_r,
    nb_s,
    nb_r,
    x_s,
    x_r,
    opp_sb,
    opp_rb,
    nb_sb,
    nb_rb,
    x_sb,
    x_rb,
    pre,
    rkeep,
    ropp_s,
    ropp_r,
    rnb_s,
    rnb_r,
    rx_s,
    rx_r,
    rres,
    own_tan,
    w_sem,
    d_send,
    d_recv,
    c_send,
    c_recv,
    cb_send,
    cb_recv,
    g_send,
    g_recv,
    gb_send,
    gb_recv,
    r_send,
    r_recv,
    s_send,
    s_recv,
):
    r, c = lax.axis_index("row"), lax.axis_index("col")
    z, x_lo = r // 2, r % 2
    y, x_hi, core = c // 4, (c // 2) % 2, c % 2
    core_mate = (r, c + 1 - 2 * core)
    x_mate = (r, c + 2 - 4 * x_hi)
    y_plus, y_minus = (r, lax.rem(c + 4, 16)), (r, lax.rem(c + 12, 16))
    z_plus, z_minus = (lax.rem(r + 2, 8), c), (lax.rem(r + 6, 8), c)
    lo_mate = (r + 1 - 2 * x_lo, c)

    def weight_copy(j, which):
        cols = pl.ds(pl.multiple_of(j * CW, CW), CW)
        src, dst = (gate_hbm, wg) if which == 0 else (up_hbm, wu)
        return pltpu.make_async_copy(src.at[:, cols], dst.at[:, cols], w_sem.at[which, j])

    def down_copy():
        return pltpu.make_async_copy(down_hbm, wd, w_sem.at[0, NJ])

    def start_weights(j, _):
        weight_copy(j, 0).start()
        weight_copy(j, 1).start()
        return 0

    lax.fori_loop(0, NJ, start_weights, 0)

    barrier = pltpu.get_barrier_semaphore()
    mates = (core_mate, x_mate, y_plus, y_minus, z_plus, z_minus, lo_mate)
    for dev in mates:
        pl.semaphore_signal(barrier, inc=1, device_id=dev, device_id_type=MESH)

    own_rows = pl.multiple_of(r * 32, 32)
    lhs[1, pl.ds(own_rows, 32), :] = tok_ref[...]
    pl.semaphore_wait(barrier, len(mates))

    def tok_region(k, at, rows, half):
        if half is None:
            return lhs.at[1, pl.ds(at, rows), :]
        return lhs.at[1, pl.ds(at, rows), pl.ds(half * (KD // 2), KD // 2)]

    def cot_region(k, at, rows, half):
        cols = pl.ds(pl.multiple_of(k * CW, CW), CW)
        if half is None:
            return cot.at[:, pl.ds(at, rows), cols]
        return cot.at[pl.ds(half, 1), pl.ds(at, rows), cols]

    def wide_region(ref):
        def region(k, at, rows, half):
            cols = pl.ds(pl.multiple_of(k * CW, CW), CW)
            if half is None:
                return ref.at[:, pl.ds(at, rows), cols]
            return ref.at[pl.ds(half, 1), pl.ds(at, rows), cols]

        return region

    tok_spread = Spread(z, z_plus, z_minus, lo_mate, x_lo, 64, 0, tok_region, (s_send, s_recv))
    cot_spread = Spread(z, z_plus, z_minus, lo_mate, x_lo, 64, 0, cot_region, (s_send, s_recv))
    hid_spread = Spread(y, y_plus, y_minus, x_mate, x_hi, 32, core * 128, wide_region(hid), (g_send, g_recv))
    back_spread = Spread(y, y_plus, y_minus, x_mate, x_hi, 32, core * 128, wide_region(back), (gb_send, gb_recv))
    pre_ring = Ring(
        y, y_plus, y_minus, x_mate, x_hi, 32, (log_encode, log_decode),
        (opp_s, opp_r, nb_s, nb_r, x_s, x_r, keep), (c_send, c_recv), (log_encode, log_decode),
    )
    back_ring = Ring(
        y, y_plus, y_minus, x_mate, x_hi, 32, (bf_encode, bf_decode),
        (opp_sb, opp_rb, nb_sb, nb_rb, x_sb, x_rb, keep), (cb_send, cb_recv), (bf_encode, bf_decode),
    )
    row_ring = Ring(
        z, z_plus, z_minus, lo_mate, x_lo, 64, (bf_encode, bf_decode),
        (ropp_s, ropp_r, rnb_s, rnb_r, rx_s, rx_r, rkeep), (r_send, r_recv), (lambda v: v, lambda v: v),
    )

    tok_spread.first(NF)

    words = words_ref[...]
    parts = [lax.shift_right_logical(words, jnp.full_like(words, 8 * b)) & 255 for b in range(4)]
    octets = jnp.concatenate(parts, axis=0).astype(F32).astype(BF16)
    at = lax.broadcasted_iota(I32, (128, KD), 0)
    lane = lax.broadcasted_iota(I32, (128, KD), 1)
    pick = ((at % 32) * 4 + at // 32 == lane // 8).astype(F32).astype(BF16)
    spread = lax.dot_general(octets, pick, (((0,), (0,)), ((), ())), preferred_element_type=F32)
    bit = lax.broadcasted_iota(I32, (TOK, KD), 1) % 8
    signs = 2 * (lax.shift_right_logical(spread.astype(I32), bit) & 1) - 1
    lhs[0] = signs.astype(F32).astype(BF16)

    core_rows = pl.multiple_of(core * 128, 128)
    mate_rows = pl.multiple_of((1 - core) * 128, 128)
    share_rows = pl.multiple_of(core * 128 + y * 32 + x_hi * 16, 16)

    def core_copy(kk):
        sl = lax.rem(kk, 4)
        return rdma(
            res.at[sl, :, pl.ds(mate_rows, 128), :], d2d.at[kk], d_send.at[kk], d_recv.at[kk], core_mate
        )

    def wide_copy(ref, k, rows, sems):
        cols = pl.ds(pl.multiple_of(k * CW, CW), CW)
        part = ref.at[:, pl.ds(rows, 128), cols]
        return rdma(part, part, sems[0].at[k, 5], sems[1].at[k, 5], core_mate)

    def chip_term(kk):
        sl = lax.rem(kk, 4)

        def term(block, p):
            rows = pl.multiple_of(core_rows + block, 32)
            return res[sl, p, pl.ds(rows, 32), :] + d2d[kk, p, pl.ds(block, 32), :]

        return term

    def stage(t, lag, low, high, work):
        k = t - lag

        @pl.when((k >= low) & (k < high))
        def _():
            work(k)

    def sweep(count, first_gather, base, multiply, ring, spreader, wide, sems, shares, extra):
        def begin(k):
            multiply(k)
            core_copy(base + k).start()

        def chip_sum(k):
            core_copy(base + k).wait()
            ring.scatter(k, chip_term(base + k))

        def shared(k):
            shares(k, ring.finish(k))

        def to_mate(j):
            spreader.last(j)
            wide_copy(wide, j, core_rows, sems).start()

        def from_mate(j):
            wide_copy(wide, j, core_rows, sems).wait_send()
            wide_copy(wide, j, mate_rows, sems).wait_recv()

        def step(t, _):
            gt = t - first_gather
            stage(gt, LAG[8], 0, NJ, from_mate)
            stage(gt, LAG[7], 0, NJ, to_mate)
            stage(gt, LAG[6], 0, NJ, spreader.third)
            stage(gt, LAG[5], 0, NJ, spreader.second)
            stage(t, LAG[4], 0, count, shared)
            stage(gt, LAG[4], 0, NJ, spreader.first)
            stage(t, LAG[3], 0, count, ring.gather_in)
            stage(t, LAG[2], 0, count, ring.relay)
            stage(t, LAG[1], 0, count, chip_sum)
            if extra is not None:
                extra(t)
            stage(t, LAG[0], 0, count, begin)
            return 0

        lax.fori_loop(0, count + LAG[8], step, 0)

    def cols_of(k):
        return pl.ds(pl.multiple_of(k * CW, CW), CW)

    def multiply_in(k):
        j, which = k % NJ, k // NJ

        @pl.when(k < NJ)
        def _():
            weight_copy(j, 0).wait()
            weight_copy(j, 1).wait()

        sl = lax.rem(k, 4)
        res[sl, 0] = dot(lhs[which], wg[:, cols_of(j)])
        res[sl, 1] = dot(lhs[which], wu[:, cols_of(j)])

    def shares_in(k, sums):
        pre[k, 0] = sums[0]
        pre[k, 1] = sums[1]

        @pl.when(k >= NJ)
        def _():
            j = k - NJ
            active, slopes, _ = silu_parts(pre[k, 0])
            up_pre, gate_tan, up_tan = pre[k, 1], pre[j, 0], pre[j, 1]
            hid[0, pl.ds(share_rows, 16), cols_of(j)] = (active * up_pre).astype(BF16)
            hid[1, pl.ds(share_rows, 16), cols_of(j)] = (
                slopes * gate_tan * up_pre + active * up_tan
            ).astype(BF16)

    def token_steps(t):
        @pl.when(t == 2)
        def _():
            tok_spread.second(NF)

        @pl.when(t == 6)
        def _():
            tok_spread.third(NF)

        @pl.when(t == 9)
        def _():
            down_copy().start()

        @pl.when(t == 11)
        def _():
            tok_spread.last(NF)

    sweep(
        2 * NJ, NJ, 0, multiply_in, pre_ring, hid_spread, hid, (g_send, g_recv), shares_in, token_steps
    )
    down_copy().wait()

    def row_term(sl):
        def term(block, p):
            return rres[sl, p, pl.ds(block, 64), :]

        return term

    def multiply_out(n):
        for q in range(2):
            rres[0, q] = dot(hid[q], wd[:, cols_of(n)])
        row_ring.scatter(n, row_term(0))

    def cotangents(n):
        out, out_tan = row_ring.finish(n)
        scale = wt_ref[pl.ds(own_rows, 32), :]
        rows, cols = pl.ds(own_rows, 32), cols_of(n)
        tan = scale * (lhs[0, rows, cols].astype(F32) + out_tan)
        own_tan[:, cols] = tan
        cot[0, rows, cols] = (scale * (lhs[1, rows, cols].astype(F32) + out)).astype(BF16)
        cot[1, rows, cols] = tan.astype(BF16)
        cot_spread.first(n)

    def out_step(t, _):
        stage(t, 6, 0, NF, cot_spread.last)
        stage(t, 5, 0, NF, cot_spread.third)
        stage(t, 4, 0, NF, cot_spread.second)
        stage(t, 3, 0, NF, cotangents)
        stage(t, 2, 0, NF, row_ring.gather_in)
        stage(t, 1, 0, NF, row_ring.relay)
        stage(t, 0, 0, NF, multiply_out)
        return 0

    lax.fori_loop(0, NF + 6, out_step, 0)

    def multiply_back(k):
        sl = lax.rem(2 * NJ + k, 4)
        rows = pl.ds(pl.multiple_of(k * CW, CW), CW)
        for q in range(2):
            res[sl, q] = dot_t(cot[q], wd[rows, :])

    def shares_back(j, sums):
        backward, back_tan = sums
        active, slopes, curves = silu_parts(pre[NJ + j, 0])
        up_pre, gate_tan, up_tan = pre[NJ + j, 1], pre[j, 0], pre[j, 1]
        gate_back = (
            back_tan * up_pre * slopes + backward * up_tan * slopes + backward * up_pre * curves * gate_tan
        )
        up_back = back_tan * active + backward * slopes * gate_tan
        back[0, pl.ds(share_rows, 16), cols_of(j)] = gate_back.astype(BF16)
        back[1, pl.ds(share_rows, 16), cols_of(j)] = up_back.astype(BF16)

    sweep(
        NJ, 0, 2 * NJ, multiply_back, back_ring, back_spread, back, (gb_send, gb_recv), shares_back, None
    )

    def multiply_last(n):
        for p in range(2):
            rows = pl.ds(pl.multiple_of((n - NF) * 2 * CW + p * CW, CW), CW)
            rres[1, p] = dot_t(back[0], wg[rows, :]) + dot_t(back[1], wu[rows, :])
        row_ring.scatter(n, row_term(1))

    def finish_last(n):
        sums = row_ring.finish(n)
        for p in range(2):
            cols = pl.ds(pl.multiple_of((n - NF) * 2 * CW + p * CW, CW), CW)
            out_ref[:, cols] = own_tan[:, cols] + sums[p]

    def last_step(t, _):
        stage(t, 3 - NF, NF, NF + 2, finish_last)
        stage(t, 2 - NF, NF, NF + 2, row_ring.gather_in)
        stage(t, 1 - NF, NF, NF + 2, row_ring.relay)
        stage(t, 0 - NF, NF, NF + 2, multiply_last)
        return 0

    lax.fori_loop(0, 2 + 3, last_step, 0)


def block(tokens, words, weight_tok, gate_weight, up_weight, down_weight):
    vmem = lambda shape, dtype: pltpu.VMEM(shape, dtype)
    sem = lambda *shape: pltpu.SemaphoreType.DMA(shape)
    anywhere = pl.BlockSpec(memory_space=pl.ANY)
    inside = pl.BlockSpec(memory_space=pltpu.VMEM)
    NC = 2 * NJ
    return pl.pallas_call(
        block_kernel,
        out_shape=jax.ShapeDtypeStruct((32, KD), F32),
        in_specs=[inside, inside, inside, anywhere, anywhere, anywhere],
        out_specs=inside,
        scratch_shapes=[
            vmem((KD, HW), BF16),
            vmem((KD, HW), BF16),
            vmem((HW, KD), BF16),
            vmem((2, TOK, KD), BF16),
            vmem((2, TOK, KD), BF16),
            vmem((2, TOK, HW), BF16),
            vmem((2, TOK, HW), BF16),
            vmem((4, 2, TOK, CW), F32),
            vmem((NC + NJ, 2, 128, CW), F32),
            vmem((SLOTS, 4, 32, CW), F32),
            vmem((SLOTS, 2, 32, CW), I16),
            vmem((NC, 2, 32, CW), I16),
            vmem((SLOTS, 2, 2, 32, CW), I16),
            vmem((NC, 2, 2, 32, CW), I16),
            vmem((SLOTS, 2, 16, CW), I16),
            vmem((NC, 2, 16, CW), I16),
            vmem((SLOTS, 2, 32, CW), BF16),
            vmem((NJ, 2, 32, CW), BF16),
            vmem((SLOTS, 2, 2, 32, CW), BF16),
            vmem((NJ, 2, 2, 32, CW), BF16),
            vmem((SLOTS, 2, 16, CW), BF16),
            vmem((NJ, 2, 16, CW), BF16),
            vmem((NC, 2, 16, CW), F32),
            vmem((SLOTS, 4, 64, CW), F32),
            vmem((SLOTS, 2, 64, CW), BF16),
            vmem((NF + 2, 2, 64, CW), BF16),
            vmem((SLOTS, 2, 2, 64, CW), BF16),
            vmem((NF + 2, 2, 2, 64, CW), BF16),
            vmem((SLOTS, 2, 32, CW), F32),
            vmem((NF + 2, 2, 32, CW), F32),
            vmem((2, 2, TOK, CW), F32),
            vmem((32, KD), F32),
            sem(2, NJ + 1),
            sem(NC + NJ),
            sem(NC + NJ),
            sem(NC, 5),
            sem(NC, 5),
            sem(NJ, 5),
            sem(NJ, 5),
            sem(NJ, 6),
            sem(NJ, 6),
            sem(NJ, 6),
            sem(NJ, 6),
            sem(NF + 2, 5),
            sem(NF + 2, 5),
            sem(NF + 1, 5),
            sem(NF + 1, 5),
        ],
        compiler_params=pltpu.CompilerParams(
            collective_id=0, has_side_effects=True, vmem_limit_bytes=67043328
        ),
    )(tokens, words, weight_tok, gate_weight, up_weight, down_weight)


def on_device(tokens, probe_words, token_ids, loss_weight, gate_weight, up_weight, down_weight):
    weight_tok = jnp.take(loss_weight, token_ids)[:, None]
    return block(tokens, probe_words.T, weight_tok, gate_weight, up_weight, down_weight)


def solution(mesh):
    return jax.shard_map(
        on_device,
        mesh=mesh,
        in_specs=(
            P("row", "col"),
            P(None, "col"),
            P(),
            P(),
            P("col", "row"),
            P("col", "row"),
            P("row", "col"),
        ),
        out_specs=P("row", "col"),
        check_vma=False,
    )
```

```python
import functools
import math

import jax
import jax.numpy as jnp
from jax import lax
from jax.experimental import pallas as pl
from jax.experimental.pallas import tpu as pltpu
from jax.sharding import PartitionSpec as P

MESH = pl.DeviceIdType.MESH
F32, BF16, I16, I32 = jnp.float32, jnp.bfloat16, jnp.int16, jnp.int32

TOK = 256
KD = 1024
HW = 3328
CW = 256
NJ = HW // CW
NF = KD // CW
PAIRS = (NJ + 1) // 2
HP = HW + CW
LAG = (0, 1, 3, 5, 7, 9, 11, 13, 14)
NS = 4
NK = 8

CODE_UNIT = 1024.0
CODE_SCALE = 32700.0 / math.log1p(4700.0 * CODE_UNIT)


def log_encode(x):
    mag = jnp.log(1.0 + jnp.abs(x) * CODE_UNIT) * CODE_SCALE
    q = (mag + 0.5).astype(I32)
    return jnp.where(x < 0, -q, q).astype(I16)


def log_decode(y):
    y = y.astype(I32).astype(F32)
    mag = (jnp.exp(jnp.abs(y) * (1.0 / CODE_SCALE)) - 1.0) * (1.0 / CODE_UNIT)
    return jnp.where(y < 0, -mag, mag)


def bf_encode(x):
    return x.astype(BF16)


def bf_decode(x):
    return x.astype(F32)


def dot(a, b):
    return jnp.dot(a, b, preferred_element_type=F32)


def dot_t(a, b):
    return lax.dot_general(a, b, (((1,), (1,)), ((), ())), preferred_element_type=F32)


def silu_parts(pre_act):
    sig = 1.0 / (1.0 + jnp.exp(-pre_act))
    active = pre_act * sig
    slopes = sig * (1.0 + pre_act * (1.0 - sig))
    curves = sig * (1.0 - sig) * (2.0 + pre_act * (1.0 - 2.0 * sig))
    return active, slopes, curves


def rdma(src, dst, ssem, rsem, dev):
    return pltpu.make_async_remote_copy(
        src_ref=src, dst_ref=dst, send_sem=ssem, recv_sem=rsem, device_id=dev, device_id_type=MESH
    )


class Ring:
    def __init__(self, pos, plus, minus, mate, side, rows, arrays, code, bufs, sems, x_code):
        self.pos, self.plus, self.minus, self.mate, self.side = pos, plus, minus, mate, side
        self.rows, self.half = rows, rows // 2
        self.arrays, self.each = arrays, arrays // 2
        self.enc, self.dec = code
        self.x_enc, self.x_dec = x_code
        self.opp_s, self.opp_r, self.nb_s, self.nb_r, self.x_s, self.x_r, self.keep = bufs
        self.ss, self.rs = sems

    def block(self, delta):
        return pl.multiple_of(lax.rem(self.pos + (4 + delta), 4) * self.rows, self.rows)

    def opp_copy(self, k, d):
        dev = self.plus if d == 0 else self.minus
        sl, part = lax.rem(k, NS), pl.ds(d * self.each, self.each)
        return rdma(self.opp_s.at[sl, part], self.opp_r.at[sl, part], self.ss.at[sl, d], self.rs.at[sl, d], dev)

    def nb_copy(self, k, d):
        dev = self.plus if d == 0 else self.minus
        sl = lax.rem(k, NS)
        return rdma(self.nb_s.at[sl, d], self.nb_r.at[sl, d], self.ss.at[sl, 2 + d], self.rs.at[sl, 2 + d], dev)

    def x_copy(self, k):
        sl = lax.rem(k, NS)
        return rdma(self.x_s.at[sl], self.x_r.at[sl], self.ss.at[sl, 4], self.rs.at[sl, 4], self.mate)

    def scatter(self, k, term):
        sl, kp = lax.rem(k, NS), lax.rem(k, NK)
        for d in range(2):
            for i in range(d * self.each, (d + 1) * self.each):
                self.opp_s[sl, i] = self.enc(term(self.block(2), i))
            self.opp_copy(k, d).start()
        for i in range(self.arrays):
            d = i // self.each
            near, far = (1, -1) if d == 0 else (-1, 1)
            self.keep[kp, i] = term(self.block(near), i)
            self.nb_s[sl, 1 - d, i] = self.enc(term(self.block(far), i))
            self.keep[kp, self.arrays + i] = term(self.block(0), i)

    def relay(self, k):
        sl, kp = lax.rem(k, NS), lax.rem(k, NK)
        for d in range(2):
            self.opp_copy(k, d).wait()
            for i in range(d * self.each, (d + 1) * self.each):
                self.nb_s[sl, d, i] = self.enc(self.keep[kp, i] + self.dec(self.opp_r[sl, i]))
            self.nb_copy(k, d).start()

    def gather_in(self, k):
        sl, kp = lax.rem(k, NS), lax.rem(k, NK)
        for d in range(2):
            self.nb_copy(k, d).wait()
        other = pl.multiple_of((1 - self.side) * self.half, self.half)
        for i in range(self.arrays):
            own = self.arrays + i
            self.keep[kp, own] += self.dec(self.nb_r[sl, 0, i]) + self.dec(self.nb_r[sl, 1, i])
            self.x_s[sl, i] = self.x_enc(self.keep[kp, own, pl.ds(other, self.half), :])
        self.x_copy(k).start()

    def finish(self, k):
        sl, kp = lax.rem(k, NS), lax.rem(k, NK)
        self.x_copy(k).wait()
        own = pl.multiple_of(self.side * self.half, self.half)
        return [
            self.keep[kp, self.arrays + i, pl.ds(own, self.half), :] + self.x_dec(self.x_r[sl, i])
            for i in range(self.arrays)
        ]


class Spread:
    def __init__(self, pos, plus, minus, mate, side, rows, base, region, sems, slot):
        self.pos, self.plus, self.minus, self.mate, self.side = pos, plus, minus, mate, side
        self.rows, self.half, self.base, self.region = rows, rows // 2, base, region
        self.ss, self.rs = sems
        self.slot = slot

    def start_of(self, delta):
        return pl.multiple_of(self.base + lax.rem(self.pos + (4 + delta), 4) * self.rows, self.rows)

    def copy(self, k, i, ref, dev):
        sl = self.slot(k)
        return rdma(ref, ref, self.ss.at[sl, i], self.rs.at[sl, i], dev)

    def mine(self, k):
        at = pl.multiple_of(self.start_of(0) + self.side * self.half, self.half)
        return self.copy(k, 0, self.region(k, at, self.half, None), self.mate)

    def first(self, k):
        self.mine(k).start()

    def second(self, k):
        self.mine(k).wait_send()
        at = pl.multiple_of(self.start_of(0) + (1 - self.side) * self.half, self.half)
        self.copy(k, 0, self.region(k, at, self.half, None), self.mate).wait_recv()
        ref = self.region(k, self.start_of(0), self.rows, None)
        self.copy(k, 1, ref, self.plus).start()
        self.copy(k, 2, ref, self.minus).start()

    def third(self, k):
        ref = self.region(k, self.start_of(0), self.rows, None)
        self.copy(k, 1, ref, self.plus).wait_send()
        self.copy(k, 2, ref, self.minus).wait_send()
        self.copy(k, 1, self.region(k, self.start_of(-1), self.rows, None), self.plus).wait_recv()
        self.copy(k, 3, self.region(k, self.start_of(-1), self.rows, 0), self.plus).start()
        self.copy(k, 2, self.region(k, self.start_of(1), self.rows, None), self.minus).wait_recv()
        self.copy(k, 4, self.region(k, self.start_of(1), self.rows, 1), self.minus).start()

    def last(self, k):
        self.copy(k, 3, self.region(k, self.start_of(-1), self.rows, 0), self.plus).wait_send()
        self.copy(k, 4, self.region(k, self.start_of(1), self.rows, 1), self.minus).wait_send()
        self.copy(k, 3, self.region(k, self.start_of(2), self.rows, 0), self.plus).wait_recv()
        self.copy(k, 4, self.region(k, self.start_of(2), self.rows, 1), self.minus).wait_recv()


def block_kernel(
    tok_ref,
    words_ref,
    ids_ref,
    loss_hbm,
    gate_hbm,
    up_hbm,
    down_hbm,
    out_ref,
    wg,
    wu,
    wd,
    loss,
    scale,
    lhs,
    cot,
    hid,
    back,
    res,
    d2d,
    keep,
    opp_s,
    opp_r,
    nb_s,
    nb_r,
    x_s,
    x_r,
    opp_sb,
    opp_rb,
    nb_sb,
    nb_rb,
    x_sb,
    x_rb,
    pre,
    rkeep,
    ropp_s,
    ropp_r,
    rnb_s,
    rnb_r,
    rx_s,
    rx_r,
    fkeep,
    fopp_s,
    fopp_r,
    fnb_s,
    fnb_r,
    fx_s,
    fx_r,
    rres,
    own_tan,
    w_sem,
    d_send,
    d_recv,
    c_send,
    c_recv,
    g_send,
    g_recv,
    r_send,
    r_recv,
    s_send,
    s_recv,
):
    r, c = lax.axis_index("row"), lax.axis_index("col")
    z, x_lo = r // 2, r % 2
    y, x_hi, core = c // 4, (c // 2) % 2, c % 2
    core_mate = (r, c + 1 - 2 * core)
    x_mate = (r, c + 2 - 4 * x_hi)
    y_plus, y_minus = (r, lax.rem(c + 4, 16)), (r, lax.rem(c + 12, 16))
    z_plus, z_minus = (lax.rem(r + 2, 8), c), (lax.rem(r + 6, 8), c)
    lo_mate = (r + 1 - 2 * x_lo, c)

    barrier = pltpu.get_barrier_semaphore()
    mates = (core_mate, x_mate, y_plus, y_minus, z_plus, z_minus, lo_mate)
    for dev in mates:
        pl.semaphore_signal(barrier, inc=1, device_id=dev, device_id_type=MESH)

    def weight_copy(j, which):
        cols = pl.ds(pl.multiple_of(j * CW, CW), CW)
        src, dst = (gate_hbm, wg) if which == 0 else (up_hbm, wu)
        return pltpu.make_async_copy(src.at[:, cols], dst.at[:, cols], w_sem.at[which, j])

    def down_copy():
        return pltpu.make_async_copy(down_hbm, wd, w_sem.at[0, NJ])

    def loss_copy():
        return pltpu.make_async_copy(loss_hbm, loss, w_sem.at[1, NJ])

    def start_weights(j, _):
        weight_copy(j, 0).start()
        weight_copy(j, 1).start()
        return 0

    lax.fori_loop(0, NJ, start_weights, 0)
    loss_copy().start()

    own_rows = pl.multiple_of(r * 32, 32)
    lhs[1, pl.ds(own_rows, 32), :] = tok_ref[...]
    hid[:, :, :CW] = jnp.zeros((2, TOK, CW), BF16)
    back[:, :, :CW] = jnp.zeros((2, TOK, CW), BF16)

    words = words_ref[...]
    parts = [lax.shift_right_logical(words, jnp.full_like(words, 8 * b)) & 255 for b in range(4)]
    octets = jnp.concatenate(parts, axis=0).astype(F32).astype(BF16)
    at = lax.broadcasted_iota(I32, (128, KD), 0)
    lane = lax.broadcasted_iota(I32, (128, KD), 1)
    pick = ((at % 32) * 4 + at // 32 == lane // 8).astype(F32).astype(BF16)
    spread = lax.dot_general(octets, pick, (((0,), (0,)), ((), ())), preferred_element_type=F32)
    bit = lax.broadcasted_iota(I32, (TOK, KD), 1) % 8
    signs = 2 * (lax.shift_right_logical(spread.astype(I32), bit) & 1) - 1
    lhs[0] = signs.astype(F32).astype(BF16)

    pl.semaphore_wait(barrier, len(mates))

    def tok_region(k, at, rows, half):
        if half is None:
            return lhs.at[1, pl.ds(at, rows), :]
        return lhs.at[1, pl.ds(at, rows), pl.ds(half * (KD // 2), KD // 2)]

    def wide_region(ref, first, width):
        def region(k, at, rows, half):
            cols = pl.ds(pl.multiple_of((k - first) * width, width), width)
            if half is None:
                return ref.at[:, pl.ds(at, rows), cols]
            return ref.at[pl.ds(half, 1), pl.ds(at, rows), cols]

        return region

    def along_z(region, slot):
        return Spread(z, z_plus, z_minus, lo_mate, x_lo, 64, 0, region, (s_send, s_recv), slot)

    def along_y(region):
        return Spread(
            y, y_plus, y_minus, x_mate, x_hi, 32, core * 128, region, (g_send, g_recv), lambda k: lax.rem(k, NS)
        )

    tok_spread = along_z(tok_region, lambda k: NF)
    cot_spread = along_z(wide_region(cot, 0, CW), lambda k: k)
    hid_spread = along_y(wide_region(hid, 0, 2 * CW))
    back_spread = along_y(wide_region(back, PAIRS, 2 * CW))
    log_code, bf_code, plain = (log_encode, log_decode), (bf_encode, bf_decode), (lambda v: v, lambda v: v)
    y_axis, z_axis = (y, y_plus, y_minus, x_mate, x_hi), (z, z_plus, z_minus, lo_mate, x_lo)
    pre_ring = Ring(
        *y_axis, 32, 4, log_code, (opp_s, opp_r, nb_s, nb_r, x_s, x_r, keep), (c_send, c_recv), log_code
    )
    back_ring = Ring(
        *y_axis, 32, 4, bf_code, (opp_sb, opp_rb, nb_sb, nb_rb, x_sb, x_rb, keep), (c_send, c_recv), bf_code
    )
    row_ring = Ring(
        *z_axis, 64, 2, bf_code, (ropp_s, ropp_r, rnb_s, rnb_r, rx_s, rx_r, rkeep), (r_send, r_recv), plain
    )
    last_ring = Ring(
        *z_axis, 64, 2, bf_code, (fopp_s, fopp_r, fnb_s, fnb_r, fx_s, fx_r, fkeep), (r_send, r_recv), plain
    )

    tok_spread.first(NF)

    core_rows = pl.multiple_of(core * 128, 128)
    mate_rows = pl.multiple_of((1 - core) * 128, 128)
    share_rows = pl.multiple_of(core * 128 + y * 32 + x_hi * 16, 16)

    def core_copy(k):
        sl = lax.rem(k, NS)
        return rdma(res.at[sl, :, pl.ds(mate_rows, 128), :], d2d.at[sl], d_send.at[sl], d_recv.at[sl], core_mate)

    def wide_copy(spreader, k, rows):
        part = spreader.region(k, rows, 128, None)
        sl = spreader.slot(k)
        return rdma(part, part, g_send.at[sl, 5], g_recv.at[sl, 5], core_mate)

    def chip_term(k):
        sl = lax.rem(k, NS)

        def term(block, p):
            rows = pl.multiple_of(core_rows + block, 32)
            return res[sl, p, pl.ds(rows, 32), :] + d2d[sl, p, pl.ds(block, 32), :]

        return term

    def stage(t, lag, low, high, work):
        k = t - lag

        @pl.when((k >= low) & (k < high))
        def _():
            work(k)

    def sweep(low, high, shift, multiply, ring, spreader, shares, extra):
        def begin(k):
            multiply(k)
            core_copy(k).start()

        def chip_sum(k):
            core_copy(k).wait()
            ring.scatter(k, chip_term(k))

        def shared(k):
            shares(k, ring.finish(k))

        def first(k):
            spreader.first(k - shift)

        def second(k):
            spreader.second(k - shift)

        def third(k):
            spreader.third(k - shift)

        def to_mate(k):
            spreader.last(k - shift)
            wide_copy(spreader, k - shift, core_rows).start()

        def from_mate(k):
            wide_copy(spreader, k - shift, core_rows).wait_send()
            wide_copy(spreader, k - shift, mate_rows).wait_recv()

        start = high - PAIRS

        def step(t, _):
            stage(t, LAG[0], low, high, begin)
            if extra is not None:
                extra(t)
            stage(t, LAG[8], start, high, from_mate)
            stage(t, LAG[7], start, high, to_mate)
            stage(t, LAG[6], start, high, third)
            stage(t, LAG[5], start, high, second)
            stage(t, LAG[4], low, high, shared)
            stage(t, LAG[4], start, high, first)
            stage(t, LAG[3], low, high, ring.gather_in)
            stage(t, LAG[2], low, high, ring.relay)
            stage(t, LAG[1], low, high, chip_sum)
            return 0

        lax.fori_loop(low, high + LAG[8], step, 0)

    def cols_of(k):
        return pl.ds(pl.multiple_of(k * CW, CW), CW)

    def multiply_in(k):
        sl = lax.rem(k, NS)
        for u in range(2):
            n = 2 * k + u
            which, j = n // NJ, n % NJ

            @pl.when(n < NJ)
            def _():
                weight_copy(j, 0).wait()
                weight_copy(j, 1).wait()

            res[sl, 2 * u] = dot(lhs[which], wg[:, cols_of(j)])
            res[sl, 2 * u + 1] = dot(lhs[which], wu[:, cols_of(j)])

    def shares_in(k, sums):
        for u in range(2):
            n = 2 * k + u
            pre[n, 0] = sums[2 * u]
            pre[n, 1] = sums[2 * u + 1]

            @pl.when(n >= NJ)
            def _():
                j = n - NJ
                active, slopes, _ = silu_parts(pre[n, 0])
                up_pre, gate_tan, up_tan = pre[n, 1], pre[j, 0], pre[j, 1]
                hid[0, pl.ds(share_rows, 16), cols_of(j + 1)] = (active * up_pre).astype(BF16)
                hid[1, pl.ds(share_rows, 16), cols_of(j + 1)] = (
                    slopes * gate_tan * up_pre + active * up_tan
                ).astype(BF16)

    def loss_of_tokens():
        loss_copy().wait()
        lanes = lax.broadcasted_iota(I32, (1, 128), 1)

        def one(i, _):
            tid = ids_ref[own_rows + i]
            line = loss[pl.ds(tid // 128, 1), :]
            value = jnp.sum(jnp.where(lanes == tid % 128, line, 0.0), axis=1, keepdims=True)
            scale[pl.ds(i, 1), :] = jnp.broadcast_to(value, (1, 128))
            return 0

        lax.fori_loop(0, 32, one, 0)

    def token_steps(t):
        @pl.when(t == 1)
        def _():
            tok_spread.second(NF)

        @pl.when(t == 3)
        def _():
            tok_spread.third(NF)

        @pl.when(t == 5)
        def _():
            down_copy().start()
            tok_spread.last(NF)

        @pl.when(t == NJ)
        def _():
            loss_of_tokens()

    sweep(0, NJ, NJ - PAIRS, multiply_in, pre_ring, hid_spread, shares_in, token_steps)
    down_copy().wait()

    def multiply_out(n):
        for q in range(2):
            rres[q] = dot(hid[q, :, CW:], wd[:, cols_of(n)])
        row_ring.scatter(n, lambda block, p: rres[p, pl.ds(block, 64), :])

    def cotangents(n):
        out, out_tan = row_ring.finish(n)
        weight = scale[:, :1]
        rows, cols = pl.ds(own_rows, 32), cols_of(n)
        tan = weight * (lhs[0, rows, cols].astype(F32) + out_tan)
        own_tan[:, cols] = tan
        cot[0, rows, cols] = (weight * (lhs[1, rows, cols].astype(F32) + out)).astype(BF16)
        cot[1, rows, cols] = tan.astype(BF16)
        cot_spread.first(n)

    def out_step(t, _):
        stage(t, 0, 0, NF, multiply_out)
        stage(t, 12, 0, NF, cot_spread.last)
        stage(t, 10, 0, NF, cot_spread.third)
        stage(t, 8, 0, NF, cot_spread.second)
        stage(t, 6, 0, NF, cotangents)
        stage(t, 4, 0, NF, row_ring.gather_in)
        stage(t, 2, 0, NF, row_ring.relay)
        return 0

    lax.fori_loop(0, NF + 12, out_step, 0)

    def multiply_back(k):
        sl = lax.rem(k, NS)
        for u in range(2):
            j = jnp.maximum(2 * (k - NJ) - 1 + u, 0)
            rows = pl.ds(pl.multiple_of(j * CW, CW), CW)
            for q in range(2):
                res[sl, 2 * u + q] = dot_t(cot[q], wd[rows, :])

    def shares_back(k, sums):
        for u in range(2):
            j = 2 * (k - NJ) - 1 + u
            backward, back_tan = sums[2 * u], sums[2 * u + 1]

            @pl.when(j >= 0)
            def _():
                active, slopes, curves = silu_parts(pre[NJ + j, 0])
                up_pre, gate_tan, up_tan = pre[NJ + j, 1], pre[j, 0], pre[j, 1]
                gate_back = (
                    back_tan * up_pre * slopes
                    + backward * up_tan * slopes
                    + backward * up_pre * curves * gate_tan
                )
                up_back = back_tan * active + backward * slopes * gate_tan
                back[0, pl.ds(share_rows, 16), cols_of(j + 1)] = gate_back.astype(BF16)
                back[1, pl.ds(share_rows, 16), cols_of(j + 1)] = up_back.astype(BF16)

    sweep(NJ, NJ + PAIRS, NJ - PAIRS, multiply_back, back_ring, back_spread, shares_back, None)

    def multiply_last(n):
        rows = pl.ds(pl.multiple_of(n * CW, CW), CW)
        rres[0] = dot_t(back[0, :, CW:], wg[rows, :]) + dot_t(back[1, :, CW:], wu[rows, :])
        last_ring.scatter(n, lambda block, p: rres[0, pl.ds(block, 64), p * 128 : (p + 1) * 128])

    def finish_last(n):
        sums = last_ring.finish(n)
        for p in range(2):
            cols = pl.ds(pl.multiple_of(n * CW + p * 128, 128), 128)
            out_ref[:, cols] = own_tan[:, cols] + sums[p]

    def last_step(t, _):
        stage(t, 0, 0, NF, multiply_last)
        stage(t, 6, 0, NF, finish_last)
        stage(t, 4, 0, NF, last_ring.gather_in)
        stage(t, 2, 0, NF, last_ring.relay)
        return 0

    lax.fori_loop(0, NF + 6, last_step, 0)


def ring_buffers(arrays, rows, width, dtype, x_dtype):
    half = rows // 2
    shapes = ((arrays, rows), (arrays, rows), (2, arrays, rows), (2, arrays, rows))
    return [pltpu.VMEM((NS, *shape, width), dtype) for shape in shapes] + [
        pltpu.VMEM((NS, arrays, half, width), x_dtype) for _ in range(2)
    ]


def block(tokens, words, token_ids, loss_weight, gate_weight, up_weight, down_weight):
    vmem = lambda shape, dtype: pltpu.VMEM(shape, dtype)
    sem = lambda *shape: pltpu.SemaphoreType.DMA(shape)
    anywhere = pl.BlockSpec(memory_space=pl.ANY)
    inside = pl.BlockSpec(memory_space=pltpu.VMEM)
    scalars = pl.BlockSpec(memory_space=pltpu.SMEM)
    return pl.pallas_call(
        block_kernel,
        out_shape=jax.ShapeDtypeStruct((32, KD), F32),
        in_specs=[inside, inside, scalars, anywhere, anywhere, anywhere, anywhere],
        out_specs=inside,
        scratch_shapes=[
            vmem((KD, HW), BF16),
            vmem((KD, HW), BF16),
            vmem((HW, KD), BF16),
            vmem(loss_weight.shape, F32),
            vmem((32, 128), F32),
            vmem((2, TOK, KD), BF16),
            vmem((2, TOK, KD), BF16),
            vmem((2, TOK, HP), BF16),
            vmem((2, TOK, HP), BF16),
            vmem((NS, 4, TOK, CW), F32),
            vmem((NS, 4, 128, CW), F32),
            vmem((NK, 8, 32, CW), F32),
            *ring_buffers(4, 32, CW, I16, I16),
            *ring_buffers(4, 32, CW, BF16, BF16),
            vmem((2 * NJ, 2, 16, CW), F32),
            vmem((NK, 4, 64, CW), F32),
            *ring_buffers(2, 64, CW, BF16, F32),
            vmem((NK, 4, 64, 128), F32),
            *ring_buffers(2, 64, 128, BF16, F32),
            vmem((2, TOK, CW), F32),
            vmem((32, KD), F32),
            sem(2, NJ + 1),
            sem(NS),
            sem(NS),
            sem(NS, 5),
            sem(NS, 5),
            sem(NS, 6),
            sem(NS, 6),
            sem(NS, 5),
            sem(NS, 5),
            sem(NF + 1, 5),
            sem(NF + 1, 5),
        ],
        compiler_params=pltpu.CompilerParams(
            collective_id=0, has_side_effects=True, vmem_limit_bytes=67043328
        ),
    )(tokens, words, token_ids, loss_weight, gate_weight, up_weight, down_weight)


def on_device(tokens, probe_words, token_ids, loss_weight, gate_weight, up_weight, down_weight):
    return block(
        tokens, probe_words.T, token_ids, loss_weight.reshape(-1, 128), gate_weight, up_weight, down_weight
    )


def solution(mesh):
    return jax.shard_map(
        on_device,
        mesh=mesh,
        in_specs=(
            P("row", "col"),
            P(None, "col"),
            P(),
            P(),
            P("col", "row"),
            P("col", "row"),
            P("row", "col"),
        ),
        out_specs=P("row", "col"),
        check_vma=False,
    )
```

```python
import functools
import math

import jax
import jax.numpy as jnp
from jax import lax
from jax.experimental import pallas as pl
from jax.experimental.pallas import tpu as pltpu
from jax.sharding import PartitionSpec as P

MESH = pl.DeviceIdType.MESH
F32, BF16, I16, I32 = jnp.float32, jnp.bfloat16, jnp.int16, jnp.int32

TOK = 256
HALF = 128
KD = 1024
HW = 3328
CW = 256
NJ = HW // CW
NF = KD // CW
GU = 4
NG = (2 * NJ + 2) // GU
WIN = NG * GU * CW
LAG = (0, 1, 3, 5, 7, 9, 11, 13, 14)
NS = 4
NK = 8

CODE_UNIT = 1024.0
CODE_SCALE = 32700.0 / math.log1p(4700.0 * CODE_UNIT)


def log_encode(x):
    mag = jnp.log(1.0 + jnp.abs(x) * CODE_UNIT) * CODE_SCALE
    q = (mag + 0.5).astype(I32)
    return jnp.where(x < 0, -q, q).astype(I16)


def log_decode(y):
    y = y.astype(I32).astype(F32)
    mag = (jnp.exp(jnp.abs(y) * (1.0 / CODE_SCALE)) - 1.0) * (1.0 / CODE_UNIT)
    return jnp.where(y < 0, -mag, mag)


def bf_encode(x):
    return x.astype(BF16)


def bf_decode(x):
    return x.astype(F32)


def dot(a, b):
    return jnp.dot(a, b, preferred_element_type=F32)


def dot_t(a, b):
    return lax.dot_general(a, b, (((1,), (1,)), ((), ())), preferred_element_type=F32)


def silu_parts(pre_act):
    sig = 1.0 / (1.0 + jnp.exp(-pre_act))
    active = pre_act * sig
    slopes = sig * (1.0 + pre_act * (1.0 - sig))
    curves = sig * (1.0 - sig) * (2.0 + pre_act * (1.0 - 2.0 * sig))
    return active, slopes, curves


def rdma(src, dst, ssem, rsem, dev):
    return pltpu.make_async_remote_copy(
        src_ref=src, dst_ref=dst, send_sem=ssem, recv_sem=rsem, device_id=dev, device_id_type=MESH
    )


class Ring:
    def __init__(self, pos, plus, minus, mate, side, rows, arrays, code, bufs, sems, x_code, base=0):
        self.pos, self.plus, self.minus, self.mate, self.side = pos, plus, minus, mate, side
        self.rows, self.half = rows, rows // 2
        self.arrays, self.each, self.base, self.own = arrays, arrays // 2, base, arrays + base
        self.enc, self.dec = code
        self.x_enc, self.x_dec = x_code
        self.opp_s, self.opp_r, self.nb_s, self.nb_r, self.x_s, self.x_r, self.keep = bufs
        self.ss, self.rs = sems

    def block(self, delta):
        return pl.multiple_of(lax.rem(self.pos + (4 + delta), 4) * self.rows, self.rows)

    def opp_copy(self, k, d):
        dev = self.plus if d == 0 else self.minus
        sl, part = lax.rem(k, NS), pl.ds(self.base + d * self.each, self.each)
        return rdma(self.opp_s.at[sl, part], self.opp_r.at[sl, part], self.ss.at[sl, d], self.rs.at[sl, d], dev)

    def nb_copy(self, k, d):
        dev = self.plus if d == 0 else self.minus
        sl, part = lax.rem(k, NS), pl.ds(self.base, self.arrays)
        return rdma(
            self.nb_s.at[sl, d, part], self.nb_r.at[sl, d, part], self.ss.at[sl, 2 + d], self.rs.at[sl, 2 + d], dev
        )

    def x_copy(self, k):
        sl, part = lax.rem(k, NS), pl.ds(self.base, self.arrays)
        return rdma(self.x_s.at[sl, part], self.x_r.at[sl, part], self.ss.at[sl, 4], self.rs.at[sl, 4], self.mate)

    def of(self, d):
        return range(self.base + d * self.each, self.base + (d + 1) * self.each)

    def scatter(self, k, term):
        sl, kp = lax.rem(k, NS), lax.rem(k, NK)
        for d in range(2):
            for i in self.of(d):
                self.opp_s[sl, i] = self.enc(term(self.block(2), i))
            self.opp_copy(k, d).start()
        for d in range(2):
            near, far = (1, -1) if d == 0 else (-1, 1)
            for i in self.of(d):
                self.keep[kp, i] = term(self.block(near), i)
                self.nb_s[sl, 1 - d, i] = self.enc(term(self.block(far), i))
                self.keep[kp, self.own + i] = term(self.block(0), i)

    def relay(self, k):
        sl, kp = lax.rem(k, NS), lax.rem(k, NK)
        for d in range(2):
            self.opp_copy(k, d).wait()
            for i in self.of(d):
                self.nb_s[sl, d, i] = self.enc(self.keep[kp, i] + self.dec(self.opp_r[sl, i]))
            self.nb_copy(k, d).start()

    def gather_in(self, k):
        sl, kp = lax.rem(k, NS), lax.rem(k, NK)
        for d in range(2):
            self.nb_copy(k, d).wait()
        other = pl.multiple_of((1 - self.side) * self.half, self.half)
        for i in range(self.base, self.own):
            own = self.own + i
            self.keep[kp, own] += self.dec(self.nb_r[sl, 0, i]) + self.dec(self.nb_r[sl, 1, i])
            self.x_s[sl, i] = self.x_enc(self.keep[kp, own, pl.ds(other, self.half), :])
        self.x_copy(k).start()

    def finish(self, k):
        sl, kp = lax.rem(k, NS), lax.rem(k, NK)
        self.x_copy(k).wait()
        own = pl.multiple_of(self.side * self.half, self.half)
        return [
            self.keep[kp, self.own + i, pl.ds(own, self.half), :] + self.x_dec(self.x_r[sl, i])
            for i in range(self.base, self.own)
        ]


class Spread:
    def __init__(self, pos, plus, minus, mate, side, rows, base, region, sems, slot):
        self.pos, self.plus, self.minus, self.mate, self.side = pos, plus, minus, mate, side
        self.rows, self.half, self.base, self.region = rows, rows // 2, base, region
        self.ss, self.rs = sems
        self.slot = slot

    def start_of(self, delta):
        return pl.multiple_of(self.base + lax.rem(self.pos + (4 + delta), 4) * self.rows, self.rows)

    def copy(self, k, i, ref, dev):
        sl = self.slot(k)
        return rdma(ref, ref, self.ss.at[sl, i], self.rs.at[sl, i], dev)

    def mine(self, k):
        at = pl.multiple_of(self.start_of(0) + self.side * self.half, self.half)
        return self.copy(k, 0, self.region(k, at, self.half, None), self.mate)

    def first(self, k):
        self.mine(k).start()

    def second(self, k):
        self.mine(k).wait_send()
        at = pl.multiple_of(self.start_of(0) + (1 - self.side) * self.half, self.half)
        self.copy(k, 0, self.region(k, at, self.half, None), self.mate).wait_recv()
        ref = self.region(k, self.start_of(0), self.rows, None)
        self.copy(k, 1, ref, self.plus).start()
        self.copy(k, 2, ref, self.minus).start()

    def third(self, k):
        ref = self.region(k, self.start_of(0), self.rows, None)
        self.copy(k, 1, ref, self.plus).wait_send()
        self.copy(k, 2, ref, self.minus).wait_send()
        self.copy(k, 1, self.region(k, self.start_of(-1), self.rows, None), self.plus).wait_recv()
        self.copy(k, 3, self.region(k, self.start_of(-1), self.rows, 0), self.plus).start()
        self.copy(k, 2, self.region(k, self.start_of(1), self.rows, None), self.minus).wait_recv()
        self.copy(k, 4, self.region(k, self.start_of(1), self.rows, 1), self.minus).start()

    def last(self, k):
        self.copy(k, 3, self.region(k, self.start_of(-1), self.rows, 0), self.plus).wait_send()
        self.copy(k, 4, self.region(k, self.start_of(1), self.rows, 1), self.minus).wait_send()
        self.copy(k, 3, self.region(k, self.start_of(2), self.rows, 0), self.plus).wait_recv()
        self.copy(k, 4, self.region(k, self.start_of(2), self.rows, 1), self.minus).wait_recv()


class ShortRing:
    def __init__(self, pos, plus, minus, mate, far_plus, far_minus, side, rows, arrays, bufs, sems):
        self.pos, self.mate, self.side = pos, mate, side
        self.near, self.far = (plus, minus), (far_plus, far_minus)
        self.rows, self.half = rows, rows // 2
        self.arrays, self.each = arrays, arrays // 2
        self.opp_s, self.opp_r, self.nb_s, self.nb_r, self.x_s, self.x_r, self.keep = bufs
        self.ss, self.rs = sems

    def block(self, delta):
        return pl.multiple_of(lax.rem(self.pos + (4 + delta), 4) * self.rows, self.rows)

    def side_rows(self, other):
        side = 1 - self.side if other else self.side
        return pl.ds(pl.multiple_of(side * self.half, self.half), self.half)

    def opp_copy(self, k, d):
        sl, part = k % NS, pl.ds(d * self.each, self.each)
        return rdma(
            self.opp_s.at[sl, part], self.opp_r.at[sl, part], self.ss.at[sl, d], self.rs.at[sl, d], self.near[d]
        )

    def nb_copy(self, k, d, other):
        sl, i = k % NS, 2 + 2 * d + other
        dev = self.far[d] if other else self.near[d]
        src = self.nb_s.at[sl, d, :, self.side_rows(other), :]
        return rdma(src, self.nb_r.at[sl, d, other], self.ss.at[sl, i], self.rs.at[sl, i], dev)

    def x_copy(self, k):
        sl = k % NS
        return rdma(self.x_s.at[sl], self.x_r.at[sl], self.ss.at[sl, 6], self.rs.at[sl, 6], self.mate)

    def of(self, d):
        return range(d * self.each, (d + 1) * self.each)

    def scatter(self, k, term):
        sl = k % NS
        for d in range(2):
            for i in self.of(d):
                self.opp_s[sl, i] = bf_encode(term(self.block(2), i))
            self.opp_copy(k, d).start()
        for d in range(2):
            near, far = (1, -1) if d == 0 else (-1, 1)
            for i in self.of(d):
                self.keep[sl, i] = term(self.block(near), i)
                self.nb_s[sl, 1 - d, i] = bf_encode(term(self.block(far), i))
                self.keep[sl, self.arrays + i] = term(self.block(0), i)
                self.x_s[sl, i] = bf_encode(self.keep[sl, self.arrays + i, self.side_rows(1), :])
        self.x_copy(k).start()

    def relay(self, k):
        sl = k % NS
        for d in range(2):
            self.opp_copy(k, d).wait()
            for i in self.of(d):
                self.nb_s[sl, d, i] = bf_encode(self.keep[sl, i] + bf_decode(self.opp_r[sl, i]))
            for other in (1, 0):
                self.nb_copy(k, d, other).start()

    def finish(self, k):
        sl = k % NS
        self.x_copy(k).wait()
        for d in range(2):
            for other in range(2):
                self.nb_copy(k, d, other).wait()
        sums = []
        for i in range(self.arrays):
            total = self.keep[sl, self.arrays + i, self.side_rows(0), :] + bf_decode(self.x_r[sl, i])
            for d in range(2):
                for other in range(2):
                    total = total + bf_decode(self.nb_r[sl, d, other, i])
            sums.append(total)
        return sums


class ShortSpread:
    def __init__(self, pos, plus, minus, mate, far_plus, far_minus, side, rows, region, sems):
        self.pos, self.side, self.rows, self.half, self.region = pos, side, rows, rows // 2, region
        self.near, self.far, self.mate = (plus, minus), (far_plus, far_minus), mate
        self.ss, self.rs = sems

    def start_of(self, delta):
        return pl.multiple_of(lax.rem(self.pos + (4 + delta), 4) * self.rows, self.rows)

    def part(self, k, delta, other):
        side = 1 - self.side if other else self.side
        return self.region(k, pl.multiple_of(self.start_of(delta) + side * self.half, self.half), self.half, None)

    def copy(self, k, i, ref, dev):
        return rdma(ref, ref, self.ss.at[k, i], self.rs.at[k, i], dev)

    def own_copies(self, k):
        mine = self.part(k, 0, 0)
        far = [self.copy(k, 3 + d, mine, self.far[d]) for d in range(2)]
        near = [self.copy(k, 1 + d, mine, self.near[d]) for d in range(2)]
        return far + near + [self.copy(k, 0, mine, self.mate)]

    def relay_copy(self, k, d):
        return self.copy(k, 5 + d, self.region(k, self.start_of(2 * d - 1), self.rows, d), self.near[d])

    def first(self, k):
        for one in self.own_copies(k):
            one.start()

    def third(self, k):
        for d in range(2):
            self.copy(k, 1 + d, self.part(k, 2 * d - 1, 0), self.near[d]).wait_recv()
            self.copy(k, 3 + d, self.part(k, 2 * d - 1, 1), self.far[d]).wait_recv()
            self.relay_copy(k, d).start()

    def last(self, k):
        for one in self.own_copies(k):
            one.wait_send()
        self.copy(k, 0, self.part(k, 0, 1), self.mate).wait_recv()
        for d in range(2):
            self.relay_copy(k, d).wait_send()
            self.copy(k, 5 + d, self.region(k, self.start_of(2), self.rows, d), self.near[d]).wait_recv()


def block_kernel(
    tok_ref,
    words_ref,
    ids_ref,
    loss_hbm,
    gate_hbm,
    up_hbm,
    down_hbm,
    tan_ref,
    out_ref,
    wg,
    wu,
    wd,
    loss,
    scale,
    lhs,
    cot,
    hid,
    back,
    res,
    d2d,
    keep,
    opp_s,
    opp_r,
    nb_s,
    nb_r,
    x_s,
    x_r,
    opp_sb,
    opp_rb,
    nb_sb,
    nb_rb,
    x_sb,
    x_rb,
    pre,
    rkeep,
    ropp_s,
    ropp_r,
    rnb_s,
    rnb_r,
    rx_s,
    rx_r,
    fkeep,
    fopp_s,
    fopp_r,
    fnb_s,
    fnb_r,
    fx_s,
    fx_r,
    acc,
    last,
    w_sem,
    d_send,
    d_recv,
    c_send,
    c_recv,
    g_send,
    g_recv,
    r_send,
    r_recv,
    s_send,
    s_recv,
):
    r, c = lax.axis_index("row"), lax.axis_index("col")
    z, x_lo = r // 2, r % 2
    y, x_hi, core = c // 4, (c // 2) % 2, c % 2
    core_mate = (r, c + 1 - 2 * core)
    x_mate = (r, c + 2 - 4 * x_hi)
    y_plus, y_minus = (r, lax.rem(c + 4, 16)), (r, lax.rem(c + 12, 16))
    z_plus, z_minus = (lax.rem(r + 2, 8), c), (lax.rem(r + 6, 8), c)
    lo_mate = (r + 1 - 2 * x_lo, c)
    far_plus, far_minus = ((lax.rem(r + 2, 8) + 1 - 2 * x_lo, c), (lax.rem(r + 6, 8) + 1 - 2 * x_lo, c))

    barrier = pltpu.get_barrier_semaphore()
    mates = (core_mate, x_mate, y_plus, y_minus, z_plus, z_minus, lo_mate, far_plus, far_minus)
    for dev in mates:
        pl.semaphore_signal(barrier, inc=1, device_id=dev, device_id_type=MESH)

    def weight_copy(j, which):
        cols = pl.ds(pl.multiple_of(j * CW, CW), CW)
        src, dst = (gate_hbm, wg) if which == 0 else (up_hbm, wu)
        return pltpu.make_async_copy(src.at[:, cols], dst.at[:, cols], w_sem.at[which, j])

    def down_copy():
        return pltpu.make_async_copy(down_hbm, wd, w_sem.at[0, NJ])

    def loss_copy():
        return pltpu.make_async_copy(loss_hbm, loss, w_sem.at[1, NJ])

    def start_weights(j, _):
        weight_copy(j, 0).start()
        weight_copy(j, 1).start()
        return 0

    lax.fori_loop(0, NJ, start_weights, 0)
    loss_copy().start()

    own_rows = pl.multiple_of(r * 32, 32)
    stream_rows = pl.multiple_of(r * 16, 16)
    for h in range(2):
        lhs[1, h, pl.ds(stream_rows, 16), :] = tok_ref[h * 16 : (h + 1) * 16, :]
    for ref in (hid, back):
        ref[:, :, : 2 * CW] = jnp.zeros((2, HALF, 2 * CW), BF16)

    words = words_ref[...]
    parts = [lax.shift_right_logical(words, jnp.full_like(words, 8 * b)) & 255 for b in range(4)]
    octets = jnp.concatenate(parts, axis=0).astype(F32).astype(BF16)
    at = lax.broadcasted_iota(I32, (128, KD), 0)
    lane = lax.broadcasted_iota(I32, (128, KD), 1)
    pick = ((at % 32) * 4 + at // 32 == lane // 8).astype(F32).astype(BF16)
    spread = lax.dot_general(octets, pick, (((0,), (0,)), ((), ())), preferred_element_type=F32)
    bit = lax.broadcasted_iota(I32, (TOK, KD), 1) % 8
    signs = 2 * (lax.shift_right_logical(spread.astype(I32), bit) & 1) - 1
    signs = signs.astype(F32).astype(BF16)
    for i in range(TOK // 16):
        lhs[0, i % 2, i // 2 * 16 : (i // 2 + 1) * 16, :] = signs[i * 16 : (i + 1) * 16]

    pl.semaphore_wait(barrier, len(mates))

    def tok_region(k, at, rows, half):
        if half is None:
            return lhs.at[1, :, pl.ds(at, rows), :]
        return lhs.at[1, :, pl.ds(at, rows), pl.ds(half * (KD // 2), KD // 2)]

    def wide_region(ref, shift, width):
        def region(k, at, rows, half):
            end = (k - shift + 1) * GU * CW
            cols = pl.ds(pl.multiple_of(end - width, width), width)
            if half is None:
                return ref.at[:, pl.ds(at, rows), cols]
            return ref.at[pl.ds(half, 1), pl.ds(at, rows), cols]

        return region

    def cot_region(k, at, rows, half):
        h, n = k // 2, k % 2
        cols = pl.ds(pl.multiple_of(n * 2 * CW, 2 * CW), 2 * CW)
        if half is None:
            return cot.at[h, :, pl.ds(at, rows), cols]
        return cot.at[h, pl.ds(half, 1), pl.ds(at, rows), cols]

    z_axis = (z, z_plus, z_minus, lo_mate, far_plus, far_minus, x_lo)

    def along_z(region):
        return ShortSpread(*z_axis, 32, region, (s_send, s_recv))

    def along_y(region):
        return Spread(
            y, y_plus, y_minus, x_mate, x_hi, 16, core * 64, region, (g_send, g_recv), lambda k: lax.rem(k, NS)
        )

    tok_spread = along_z(tok_region)
    cot_spread = along_z(cot_region)
    hid_spread = [along_y(wide_region(hid, 0, w * CW)) for w in (GU // 2, GU)]
    back_spread = [along_y(wide_region(back, NG, w * CW)) for w in (GU // 2, GU)]
    log_code, bf_code = (log_encode, log_decode), (bf_encode, bf_decode)
    y_axis = (y, y_plus, y_minus, x_mate, x_hi)
    pre_rings = [None, Ring(
        *y_axis, 16, 8, log_code, (opp_s, opp_r, nb_s, nb_r, x_s, x_r, keep), (c_send, c_recv), log_code
    )]
    back_bufs = (opp_sb, opp_rb, nb_sb, nb_rb, x_sb, x_rb, keep)
    back_rings = [
        Ring(*y_axis, 16, n, bf_code, back_bufs, (c_send, c_recv), bf_code, base=GU * 2 - n) for n in (GU, GU * 2)
    ]
    row_bufs = (ropp_s, ropp_r, rnb_s, rnb_r, rx_s, rx_r, rkeep)
    last_bufs = (fopp_s, fopp_r, fnb_s, fnb_r, fx_s, fx_r, fkeep)
    row_ring = ShortRing(*z_axis, 32, 4, row_bufs, (r_send, r_recv))
    last_ring = ShortRing(*z_axis, 32, 2, last_bufs, (r_send, r_recv))

    tok_spread.first(NF)

    core_rows = pl.multiple_of(core * 64, 64)
    mate_rows = pl.multiple_of((1 - core) * 64, 64)
    share_rows = pl.ds(pl.multiple_of(core * 64 + y * 16 + x_hi * 8, 8), 8)

    def core_copy(k, ring):
        sl, part = lax.rem(k, NS), pl.ds(ring.base, ring.arrays)
        return rdma(
            res.at[sl, part, pl.ds(mate_rows, 64), :], d2d.at[sl, part], d_send.at[sl], d_recv.at[sl], core_mate
        )

    def wide_copy(spreader, k, rows):
        part = spreader.region(k, rows, 64, None)
        sl = spreader.slot(k)
        return rdma(part, part, g_send.at[sl, 5], g_recv.at[sl, 5], core_mate)

    def chip_term(k):
        sl = lax.rem(k, NS)

        def term(block, p):
            rows = pl.multiple_of(core_rows + block, 16)
            return res[sl, p, pl.ds(rows, 16), :] + d2d[sl, p, pl.ds(block, 16), :]

        return term

    def stage(t, lag, low, high, work):
        k = t - lag

        @pl.when((k >= low) & (k < high))
        def _():
            work(k)

    def sweep(low, high, shift, multiply, rings, spreaders, shares, accumulate, extra, after, early=0):
        def either(first, pair, k, work):
            if pair[0] is None:
                work(pair[1])
                return
            for small, one in ((True, pair[0]), (False, pair[1])):

                @pl.when((k == first) == small)
                def _():
                    work(one)

        def ring_stage(work):
            return lambda k: either(low, rings, k, lambda ring: work(k, ring))

        def spread_stage(work):
            return lambda k: either(high - NG, spreaders, k, lambda one: work(k - shift, one))

        def start_core(k, ring):
            core_copy(k, ring).start()

        def chip_add(k, ring):
            core_copy(k, ring).wait()
            ring.scatter(k, chip_term(k))

        def send_wide(k, one):
            one.last(k)
            wide_copy(one, k, core_rows).start()

        def wait_wide(k, one):
            wide_copy(one, k, core_rows).wait_send()
            wide_copy(one, k, mate_rows).wait_recv()

        start_cores = ring_stage(start_core)

        def begin(k):
            multiply(k)
            start_cores(k)

        chip_sum = ring_stage(chip_add)
        relay = ring_stage(lambda k, ring: ring.relay(k))
        gather_in = ring_stage(lambda k, ring: ring.gather_in(k))
        shared = ring_stage(lambda k, ring: shares(k, ring.finish(k), ring.base // 2))
        first = spread_stage(lambda k, one: one.first(k))
        second = spread_stage(lambda k, one: one.second(k))
        third = spread_stage(lambda k, one: one.third(k))
        to_mate = spread_stage(send_wide)
        from_mate = spread_stage(wait_wide)

        start = high - NG

        def step(t, _):
            if early:
                stage(t, LAG[2], low, low + 1, relay)
            stage(t, LAG[0], low, high, begin)
            if extra is not None:
                extra(t)
            stage(t, LAG[8], start, high, from_mate)
            stage(t, LAG[7], start, high, to_mate)
            stage(t, LAG[6], start, high, third)
            stage(t, LAG[5], start, high, second)
            stage(t, LAG[4], low, high, shared)
            stage(t, LAG[4], start, high, first)
            stage(t, LAG[3], low, high, gather_in)
            stage(t, LAG[2], low + early, high, relay)
            stage(t, LAG[1], low, high, chip_sum)
            stage(t, LAG[8], start, high, lambda k: accumulate(k - start))
            for work in after:
                work(t)
            return 0

        lax.fori_loop(low, high + LAG[8], step, 0)

    def cols_of(k):
        return pl.ds(pl.multiple_of(k * CW, CW), CW)

    def multiply_in(k):
        sl = lax.rem(k, NS)

        def probe_chunk(u):
            j = 2 * k + u
            weight_copy(j, 0).wait()
            weight_copy(j, 1).wait()
            left = lhs[0].reshape(TOK, KD)
            for p, weight in enumerate((wg, wu)):
                both = dot(left, weight[:, cols_of(j)])
                res[sl, 4 * u + p] = both[:HALF]
                res[sl, 4 * u + 2 + p] = both[HALF:]

        def token_unit(i):
            v = GU * k + i - 2 * NJ
            for p, weight in enumerate((wg, wu)):
                res[sl, 2 * i + p] = dot(lhs[1, v // NJ], weight[:, cols_of(v % NJ)])

        @pl.when(k <= NJ // 2)
        def _():
            probe_chunk(0)

        @pl.when(k < NJ // 2)
        def _():
            probe_chunk(1)

        @pl.when(k == NJ // 2)
        def _():
            tok_spread.last(NF)

        @pl.when(k > NJ // 2)
        def _():
            token_unit(0)
            token_unit(1)

        @pl.when(k >= NJ // 2)
        def _():
            token_unit(2)
            token_unit(3)

    def shares_in(k, sums, skip):
        for i in range(GU):
            n = GU * k + i
            v = n - 2 * NJ

            @pl.when(v < 0)
            def _():
                at = n % 2 * NJ + n // 2
                pre[at, 0] = sums[2 * i]
                pre[at, 1] = sums[2 * i + 1]

            @pl.when(v >= 0)
            def _():
                pre[n, 0] = sums[2 * i]
                pre[n, 1] = sums[2 * i + 1]
                active, slopes, _ = silu_parts(pre[n, 0])
                up_pre, gate_tan, up_tan = pre[n, 1], pre[v, 0], pre[v, 1]
                hid[0, share_rows, cols_of(v + 2)] = (active * up_pre).astype(BF16)
                hid[1, share_rows, cols_of(v + 2)] = (slopes * gate_tan * up_pre + active * up_tan).astype(BF16)

    def loss_of_tokens():
        loss_copy().wait()
        lanes = lax.broadcasted_iota(I32, (1, 128), 1)

        for i in range(32):
            tid = ids_ref[own_rows + i]
            line = loss[pl.ds(tid // 128, 1), :]
            value = jnp.sum(jnp.where(lanes == tid % 128, line, 0.0), axis=1, keepdims=True)
            scale[i : i + 1, :] = jnp.broadcast_to(value, (1, 128))

    def token_spread(t):
        @pl.when(t == 3)
        def _():
            tok_spread.third(NF)

    def token_steps(t):
        @pl.when(t == 5)
        def _():
            down_copy().start()

        @pl.when(t == 8)
        def _():
            loss_of_tokens()

        @pl.when(t == NJ)
        def _():
            down_copy().wait()

    def gather_out(g):
        @pl.when(g == 0)
        def _():
            add_out(0, 2, 0, 2, True)

        @pl.when((g == 1) | (g == 2))
        def _():
            add_out(0, GU * g, GU * g - 2, GU, False)

        @pl.when(g == 3)
        def _():
            add_out(0, GU * 3, GU * 3 - 2, 3, False)
            add_out(1, GU * 3 + 3, 0, 1, True)

        @pl.when(g > 3)
        def _():
            add_out(1, GU * g, GU * g - 2 - NJ, GU, False)

    def gather_last(g):
        @pl.when(g == 3)
        def _():
            add_last(0, 1, True, pl.ds(0, KD))

        @pl.when((g > 3) & (g < NG - 1))
        def _():
            add_last(GU * g - 2 - NJ, GU, False, pl.ds(0, KD))

    def slices(first, j, units):
        width = units * CW
        return pl.ds(pl.multiple_of(first * CW, CW), width), pl.ds(pl.multiple_of(j * CW, CW), width)

    def add_out(h, first, j, units, opens):
        at, unit = slices(first, j, units)
        part = dot(hid[:, :, at].reshape(2 * HALF, units * CW), wd[unit, :])
        acc[h] = part if opens else acc[h] + part

    def add_last(j, units, opens, cols):
        part = 0.0
        for q, weight in enumerate((wg, wu)):
            at, unit = slices(j + 2, j, units)
            later, _ = slices(j + 2 + NJ, j, units)
            left = jnp.concatenate([back[q, :, at], back[q, :, later]], axis=0)
            part = part + dot_t(left, weight[cols, unit])
        last[:, cols] = part if opens else last[:, cols] + part

    def out_term(e):
        h, n = e // 2, e % 2

        def term(block, i):
            at = (2 * n + i // 2) * CW
            return acc[h, pl.ds(pl.multiple_of(i % 2 * HALF + block, 32), 32), at : at + CW]

        return term

    def cotangents(e):
        h, n = e // 2, e % 2
        sums = row_ring.finish(e)
        weight = scale[h * 16 : (h + 1) * 16, :1]
        rows = pl.ds(stream_rows, 16)
        for i in range(2):
            cols = cols_of(2 * n + i)
            tan = weight * (lhs[0, h, rows, cols].astype(F32) + sums[2 * i + 1])
            tan_ref[h * 16 : (h + 1) * 16, cols] = tan
            cot[h, 0, rows, cols] = (weight * (lhs[1, h, rows, cols].astype(F32) + sums[2 * i])).astype(BF16)
            cot[h, 1, rows, cols] = tan.astype(BF16)
        cot_spread.first(e)

    row_works = dict(
        S=lambda e: row_ring.scatter(e, out_term(e)),
        R=row_ring.relay,
        F=cotangents,
        T=cot_spread.third,
        L=cot_spread.last,
    )

    def in_order(works, names):
        for name in names.split():
            works[name[0]](int(name[1]))

    def at_steps(works, table):
        def steps(t):
            for step, names in table:

                @pl.when(t == step)
                def _():
                    in_order(works, names)

        return steps

    done = NJ - 4 + LAG[8]
    sweep(
        0, NJ, NJ - NG, multiply_in, pre_rings, hid_spread, shares_in, gather_out, token_steps,
        (token_spread, at_steps(row_works, ((done, "S0 S1"), (done + 2, "R0 R1"), (done + 3, "S2 S3")))),
    )
    in_order(row_works, "F0 F1 R2 R3 T0 T1 F2 L0 F3 L1")

    def multiply_back(k):
        @pl.when(k == NJ + 3)
        def _():
            cot_spread.last(2)
            cot_spread.last(3)

        sl = lax.rem(k, NS)
        for i in range(GU):
            v = jnp.maximum(GU * (k - NJ) - 2 + i, 0)
            left = cot[v // NJ].reshape(TOK, KD)
            both = dot_t(left, wd[pl.ds(pl.multiple_of(v % NJ * CW, CW), CW), :])
            res[sl, 2 * i] = both[:HALF]
            res[sl, 2 * i + 1] = both[HALF:]

    def shares_back(k, sums, skip):
        for i in range(skip, GU):
            v = GU * (k - NJ) - 2 + i
            backward, back_tan = sums[2 * (i - skip)], sums[2 * (i - skip) + 1]

            @pl.when(v >= 0)
            def _():
                active, slopes, curves = silu_parts(pre[2 * NJ + v, 0])
                up_pre, gate_tan, up_tan = pre[2 * NJ + v, 1], pre[v, 0], pre[v, 1]
                gate_back = (
                    back_tan * up_pre * slopes
                    + backward * up_tan * slopes
                    + backward * up_pre * curves * gate_tan
                )
                up_back = back_tan * active + backward * slopes * gate_tan
                back[0, share_rows, cols_of(v + 2)] = gate_back.astype(BF16)
                back[1, share_rows, cols_of(v + 2)] = up_back.astype(BF16)

    def last_term(f):
        h, n = f // 2, f % 2

        def term(block, i):
            at = (2 * n + i) * CW
            return last[pl.ds(pl.multiple_of(h * HALF + block, 32), 32), at : at + CW]

        return term

    def finish_last(f):
        h, n = f // 2, f % 2
        sums = last_ring.finish(f)
        for i in range(2):
            at = (2 * n + i) * CW
            out_ref[h * 16 : (h + 1) * 16, at : at + CW] = sums[i]

    last_works = dict(
        S=lambda f: last_ring.scatter(f, last_term(f)),
        R=last_ring.relay,
        F=finish_last,
    )

    sweep(
        NJ, NJ + NG, NJ - NG, multiply_back, back_rings, back_spread, shares_back, gather_last,
        None, (at_steps(row_works, ((NJ + 1, "T2"), (NJ + 2, "T3"))),), 1,
    )
    for n in range(2):
        add_last(GU * (NG - 1) - 2 - NJ, GU, False, pl.ds(n * KD // 2, KD // 2))
        in_order(last_works, f"S{n} S{n + 2}")
    in_order(last_works, "R0 R2 R1 R3 F0 F2 F1 F3")


def ring_buffers(arrays, rows, width, dtype, x_dtype):
    half = rows // 2
    shapes = ((arrays, rows), (arrays, rows), (2, arrays, rows), (2, arrays, rows))
    return [pltpu.VMEM((NS, *shape, width), dtype) for shape in shapes] + [
        pltpu.VMEM((NS, arrays, half, width), x_dtype) for _ in range(2)
    ]


def short_buffers(arrays, rows, width):
    half = rows // 2
    shapes = ((arrays, rows), (arrays, rows), (2, arrays, rows), (2, 2, arrays, half), (arrays, half), (arrays, half))
    return [pltpu.VMEM((NS, *shape, width), BF16) for shape in shapes]


def block(tokens, words, token_ids, loss_weight, gate_weight, up_weight, down_weight):
    vmem = lambda shape, dtype: pltpu.VMEM(shape, dtype)
    sem = lambda *shape: pltpu.SemaphoreType.DMA(shape)
    anywhere = pl.BlockSpec(memory_space=pl.ANY)
    inside = pl.BlockSpec(memory_space=pltpu.VMEM)
    scalars = pl.BlockSpec(memory_space=pltpu.SMEM)
    return pl.pallas_call(
        block_kernel,
        out_shape=[jax.ShapeDtypeStruct((32, KD), F32)] * 2,
        in_specs=[inside, inside, scalars, anywhere, anywhere, anywhere, anywhere],
        out_specs=[inside, inside],
        scratch_shapes=[
            vmem((KD, HW), BF16),
            vmem((KD, HW), BF16),
            vmem((HW, KD), BF16),
            vmem(loss_weight.shape, F32),
            vmem((32, 128), F32),
            vmem((2, 2, HALF, KD), BF16),
            vmem((2, 2, HALF, KD), BF16),
            vmem((2, HALF, WIN), BF16),
            vmem((2, HALF, WIN), BF16),
            vmem((NS, 8, HALF, CW), F32),
            vmem((NS, 8, HALF // 2, CW), F32),
            vmem((NK, 16, 16, CW), F32),
            *ring_buffers(8, 16, CW, I16, I16),
            *ring_buffers(8, 16, CW, BF16, BF16),
            vmem((4 * NJ, 2, 8, CW), F32),
            vmem((NS, 8, 32, CW), F32),
            *short_buffers(4, 32, CW),
            vmem((NS, 4, 32, CW), F32),
            *short_buffers(2, 32, CW),
            vmem((2, TOK, KD), F32),
            vmem((TOK, KD), F32),
            sem(2, NJ + 1),
            sem(NS),
            sem(NS),
            sem(NS, 5),
            sem(NS, 5),
            sem(NS, 6),
            sem(NS, 6),
            sem(NS, 7),
            sem(NS, 7),
            sem(NF + 1, 7),
            sem(NF + 1, 7),
        ],
        compiler_params=pltpu.CompilerParams(
            collective_id=0, has_side_effects=True, vmem_limit_bytes=67043328
        ),
    )(tokens, words, token_ids, loss_weight, gate_weight, up_weight, down_weight)


def on_device(tokens, probe_words, token_ids, loss_weight, gate_weight, up_weight, down_weight):
    tan, summed = block(
        tokens, probe_words.T, token_ids, loss_weight.reshape(-1, 128), gate_weight, up_weight, down_weight
    )
    return tan + summed


def solution(mesh):
    return jax.shard_map(
        on_device,
        mesh=mesh,
        in_specs=(
            P("row", "col"),
            P(None, "col"),
            P(),
            P(),
            P("col", "row"),
            P("col", "row"),
            P("row", "col"),
        ),
        out_specs=P("row", "col"),
        check_vma=False,
    )
```

```python
import functools
import math

import jax
import jax.numpy as jnp
from jax import lax
from jax.experimental import pallas as pl
from jax.experimental.pallas import tpu as pltpu
from jax.sharding import PartitionSpec as P

MESH = pl.DeviceIdType.MESH
F32, BF16, I16, I32 = jnp.float32, jnp.bfloat16, jnp.int16, jnp.int32

TOK = 256
HALF = 128
KD = 1024
HW = 3328
CW = 256
NJ = HW // CW
NF = KD // CW
GU = 4
NG = (2 * NJ + 2) // GU
WIN = NG * GU * CW
LAG = (0, 1, 3, 5, 7, 9, 11, 13, 14)
NS = 4
NK = 8

CODE_UNIT = 1024.0
CODE_SCALE = 32700.0 / math.log1p(4700.0 * CODE_UNIT)


def log_encode(x):
    mag = jnp.log(1.0 + jnp.abs(x) * CODE_UNIT) * CODE_SCALE
    q = (mag + 0.5).astype(I32)
    return jnp.where(x < 0, -q, q).astype(I16)


def log_decode(y):
    y = y.astype(I32).astype(F32)
    mag = (jnp.exp(jnp.abs(y) * (1.0 / CODE_SCALE)) - 1.0) * (1.0 / CODE_UNIT)
    return jnp.where(y < 0, -mag, mag)


def bf_encode(x):
    return x.astype(BF16)


def bf_decode(x):
    return x.astype(F32)


def dot(a, b):
    return jnp.dot(a, b, preferred_element_type=F32)


def dot_t(a, b):
    return lax.dot_general(a, b, (((1,), (1,)), ((), ())), preferred_element_type=F32)


def silu_parts(pre_act):
    sig = 1.0 / (1.0 + jnp.exp(-pre_act))
    active = pre_act * sig
    slopes = sig * (1.0 + pre_act * (1.0 - sig))
    curves = sig * (1.0 - sig) * (2.0 + pre_act * (1.0 - 2.0 * sig))
    return active, slopes, curves


def rdma(src, dst, ssem, rsem, dev):
    return pltpu.make_async_remote_copy(
        src_ref=src, dst_ref=dst, send_sem=ssem, recv_sem=rsem, device_id=dev, device_id_type=MESH
    )


class Ring:
    def __init__(self, pos, plus, minus, mate, side, rows, arrays, code, bufs, sems, x_code, base=0):
        self.pos, self.plus, self.minus, self.mate, self.side = pos, plus, minus, mate, side
        self.rows, self.half = rows, rows // 2
        self.arrays, self.each, self.base, self.own = arrays, arrays // 2, base, arrays + base
        self.enc, self.dec = code
        self.x_enc, self.x_dec = x_code
        self.opp_s, self.opp_r, self.nb_s, self.nb_r, self.x_s, self.x_r, self.keep = bufs
        self.ss, self.rs = sems

    def block(self, delta):
        return pl.multiple_of(lax.rem(self.pos + (4 + delta), 4) * self.rows, self.rows)

    def opp_copy(self, k, d):
        dev = self.plus if d == 0 else self.minus
        sl, part = lax.rem(k, NS), pl.ds(self.base + d * self.each, self.each)
        return rdma(self.opp_s.at[sl, part], self.opp_r.at[sl, part], self.ss.at[sl, d], self.rs.at[sl, d], dev)

    def nb_copy(self, k, d):
        dev = self.plus if d == 0 else self.minus
        sl, part = lax.rem(k, NS), pl.ds(self.base, self.arrays)
        return rdma(
            self.nb_s.at[sl, d, part], self.nb_r.at[sl, d, part], self.ss.at[sl, 2], self.rs.at[sl, 2], dev
        )

    def nb_wait(self, k):
        sl, part = lax.rem(k, NS), pl.ds(self.base, self.arrays)
        ref = self.nb_r.at[sl, :, part]
        rdma(ref, ref, self.ss.at[sl, 2], self.rs.at[sl, 2], self.plus).wait()

    def x_copy(self, k):
        sl, part = lax.rem(k, NS), pl.ds(self.base, self.arrays)
        return rdma(self.x_s.at[sl, part], self.x_r.at[sl, part], self.ss.at[sl, 3], self.rs.at[sl, 3], self.mate)

    def of(self, d):
        return range(self.base + d * self.each, self.base + (d + 1) * self.each)

    def scatter(self, k, term):
        sl, kp = lax.rem(k, NS), lax.rem(k, NK)
        for d in range(2):
            for i in self.of(d):
                self.opp_s[sl, i] = self.enc(term(self.block(2), i))
            self.opp_copy(k, d).start()
        for d in range(2):
            near, far = (1, -1) if d == 0 else (-1, 1)
            for i in self.of(d):
                self.keep[kp, i] = term(self.block(near), i)
                self.nb_s[sl, 1 - d, i] = self.enc(term(self.block(far), i))
                self.keep[kp, self.own + i] = term(self.block(0), i)

    def relay(self, k):
        sl, kp = lax.rem(k, NS), lax.rem(k, NK)
        for d in range(2):
            self.opp_copy(k, d).wait()
            for i in self.of(d):
                self.nb_s[sl, d, i] = self.enc(self.keep[kp, i] + self.dec(self.opp_r[sl, i]))
            self.nb_copy(k, d).start()

    def gather_in(self, k):
        sl, kp = lax.rem(k, NS), lax.rem(k, NK)
        self.nb_wait(k)
        other = pl.multiple_of((1 - self.side) * self.half, self.half)
        for i in range(self.base, self.own):
            own = self.own + i
            self.keep[kp, own] += self.dec(self.nb_r[sl, 0, i]) + self.dec(self.nb_r[sl, 1, i])
            self.x_s[sl, i] = self.x_enc(self.keep[kp, own, pl.ds(other, self.half), :])
        self.x_copy(k).start()

    def finish(self, k):
        sl, kp = lax.rem(k, NS), lax.rem(k, NK)
        self.x_copy(k).wait()
        own = pl.multiple_of(self.side * self.half, self.half)
        return [
            self.keep[kp, self.own + i, pl.ds(own, self.half), :] + self.x_dec(self.x_r[sl, i])
            for i in range(self.base, self.own)
        ]


class Spread:
    def __init__(self, pos, plus, minus, mate, side, rows, base, region, sems, slot):
        self.pos, self.plus, self.minus, self.mate, self.side = pos, plus, minus, mate, side
        self.rows, self.half, self.base, self.region = rows, rows // 2, base, region
        self.ss, self.rs = sems
        self.slot = slot

    def start_of(self, delta):
        return pl.multiple_of(self.base + lax.rem(self.pos + (4 + delta), 4) * self.rows, self.rows)

    def copy(self, k, i, ref, dev):
        sl = self.slot(k)
        return rdma(ref, ref, self.ss.at[sl, i], self.rs.at[sl, i], dev)

    def mine(self, k):
        at = pl.multiple_of(self.start_of(0) + self.side * self.half, self.half)
        return self.copy(k, 0, self.region(k, at, self.half, None), self.mate)

    def first(self, k):
        self.mine(k).start()

    def second(self, k):
        self.mine(k).wait_send()
        at = pl.multiple_of(self.start_of(0) + (1 - self.side) * self.half, self.half)
        self.copy(k, 0, self.region(k, at, self.half, None), self.mate).wait_recv()
        ref = self.region(k, self.start_of(0), self.rows, None)
        self.copy(k, 1, ref, self.plus).start()
        self.copy(k, 2, ref, self.minus).start()

    def third(self, k):
        ref = self.region(k, self.start_of(0), self.rows, None)
        self.copy(k, 1, ref, self.plus).wait_send()
        self.copy(k, 2, ref, self.minus).wait_send()
        self.copy(k, 1, self.region(k, self.start_of(-1), self.rows, None), self.plus).wait_recv()
        self.copy(k, 3, self.region(k, self.start_of(-1), self.rows, 0), self.plus).start()
        self.copy(k, 2, self.region(k, self.start_of(1), self.rows, None), self.minus).wait_recv()
        self.copy(k, 3, self.region(k, self.start_of(1), self.rows, 1), self.minus).start()

    def last(self, k):
        self.copy(k, 3, self.region(k, self.start_of(2), self.rows, None), self.plus).wait()


class ShortRing:
    def __init__(self, pos, plus, minus, mate, far_plus, far_minus, side, rows, arrays, bufs, sems):
        self.pos, self.mate, self.side = pos, mate, side
        self.near, self.far = (plus, minus), (far_plus, far_minus)
        self.rows, self.half = rows, rows // 2
        self.arrays, self.each = arrays, arrays // 2
        self.opp_s, self.opp_r, self.nb_s, self.nb_r, self.x_s, self.x_r, self.keep = bufs
        self.ss, self.rs = sems

    def block(self, delta):
        return pl.multiple_of(lax.rem(self.pos + (4 + delta), 4) * self.rows, self.rows)

    def side_rows(self, other):
        side = 1 - self.side if other else self.side
        return pl.ds(pl.multiple_of(side * self.half, self.half), self.half)

    def opp_copy(self, k, d):
        sl, part = k % NS, pl.ds(d * self.each, self.each)
        return rdma(
            self.opp_s.at[sl, part], self.opp_r.at[sl, part], self.ss.at[sl, d], self.rs.at[sl, d], self.near[d]
        )

    def nb_copy(self, k, d, other):
        sl = k % NS
        dev = self.far[d] if other else self.near[d]
        src = self.nb_s.at[sl, d, :, self.side_rows(other), :]
        return rdma(src, self.nb_r.at[sl, d, other], self.ss.at[sl, 2], self.rs.at[sl, 2], dev)

    def nb_wait(self, k):
        sl = k % NS
        rdma(self.nb_r.at[sl], self.nb_r.at[sl], self.ss.at[sl, 2], self.rs.at[sl, 2], self.mate).wait()

    def x_copy(self, k):
        sl = k % NS
        return rdma(self.x_s.at[sl], self.x_r.at[sl], self.ss.at[sl, 3], self.rs.at[sl, 3], self.mate)

    def of(self, d):
        return range(d * self.each, (d + 1) * self.each)

    def scatter(self, k, term):
        sl = k % NS
        for d in range(2):
            for i in self.of(d):
                self.opp_s[sl, i] = bf_encode(term(self.block(2), i))
            self.opp_copy(k, d).start()
        for d in range(2):
            near, far = (1, -1) if d == 0 else (-1, 1)
            for i in self.of(d):
                self.keep[sl, i] = term(self.block(near), i)
                self.nb_s[sl, 1 - d, i] = bf_encode(term(self.block(far), i))
                self.keep[sl, self.arrays + i] = term(self.block(0), i)
                self.x_s[sl, i] = bf_encode(self.keep[sl, self.arrays + i, self.side_rows(1), :])
        self.x_copy(k).start()

    def relay(self, k):
        sl = k % NS
        for d in range(2):
            self.opp_copy(k, d).wait()
            for i in self.of(d):
                self.nb_s[sl, d, i] = bf_encode(self.keep[sl, i] + bf_decode(self.opp_r[sl, i]))
            for other in (1, 0):
                self.nb_copy(k, d, other).start()

    def finish(self, k):
        sl = k % NS
        self.x_copy(k).wait()
        self.nb_wait(k)
        sums = []
        for i in range(self.arrays):
            total = self.keep[sl, self.arrays + i, self.side_rows(0), :] + bf_decode(self.x_r[sl, i])
            for d in range(2):
                for other in range(2):
                    total = total + bf_decode(self.nb_r[sl, d, other, i])
            sums.append(total)
        return sums


class ShortSpread:
    def __init__(self, pos, plus, minus, mate, far_plus, far_minus, side, rows, region, sems):
        self.pos, self.side, self.rows, self.half, self.region = pos, side, rows, rows // 2, region
        self.near, self.far, self.mate = (plus, minus), (far_plus, far_minus), mate
        self.ss, self.rs = sems

    def start_of(self, delta):
        return pl.multiple_of(lax.rem(self.pos + (4 + delta), 4) * self.rows, self.rows)

    def part(self, k, delta, other):
        side = 1 - self.side if other else self.side
        return self.region(k, pl.multiple_of(self.start_of(delta) + side * self.half, self.half), self.half, None)

    def copy(self, k, i, ref, dev):
        return rdma(ref, ref, self.ss.at[k, i // 5], self.rs.at[k, i], dev)

    def own_copies(self, k):
        mine = self.part(k, 0, 0)
        far = [self.copy(k, 3 + d, mine, self.far[d]) for d in range(2)]
        near = [self.copy(k, 1 + d, mine, self.near[d]) for d in range(2)]
        return far + near + [self.copy(k, 0, mine, self.mate)]

    def relay_copy(self, k, d):
        return self.copy(k, 5, self.region(k, self.start_of(2 * d - 1), self.rows, d), self.near[d])

    def first(self, k):
        for one in self.own_copies(k):
            one.start()

    def third(self, k):
        for d in range(2):
            self.copy(k, 1 + d, self.part(k, 2 * d - 1, 0), self.near[d]).wait_recv()
            self.copy(k, 3 + d, self.part(k, 2 * d - 1, 1), self.far[d]).wait_recv()
            self.relay_copy(k, d).start()

    def last(self, k):
        self.copy(k, 0, self.region(k, 0, 5 * self.half, None), self.mate).wait_send()
        self.copy(k, 0, self.part(k, 0, 1), self.mate).wait_recv()
        self.copy(k, 5, self.region(k, self.start_of(2), self.rows, None), self.mate).wait()


def block_kernel(
    tok_ref,
    words_ref,
    ids_ref,
    loss_hbm,
    gate_hbm,
    up_hbm,
    down_hbm,
    tan_ref,
    out_ref,
    wg,
    wu,
    wd,
    loss,
    scale,
    lhs,
    cot,
    hid,
    back,
    res,
    d2d,
    keep,
    opp_s,
    opp_r,
    nb_s,
    nb_r,
    x_s,
    x_r,
    opp_sb,
    opp_rb,
    nb_sb,
    nb_rb,
    x_sb,
    x_rb,
    pre,
    rkeep,
    ropp_s,
    ropp_r,
    rnb_s,
    rnb_r,
    rx_s,
    rx_r,
    fkeep,
    fopp_s,
    fopp_r,
    fnb_s,
    fnb_r,
    fx_s,
    fx_r,
    acc,
    last,
    w_sem,
    d_send,
    d_recv,
    c_send,
    c_recv,
    g_send,
    g_recv,
    r_send,
    r_recv,
    s_send,
    s_recv,
):
    r, c = lax.axis_index("row"), lax.axis_index("col")
    z, x_lo = r // 2, r % 2
    y, x_hi, core = c // 4, (c // 2) % 2, c % 2
    core_mate = (r, c + 1 - 2 * core)
    x_mate = (r, c + 2 - 4 * x_hi)
    y_plus, y_minus = (r, lax.rem(c + 4, 16)), (r, lax.rem(c + 12, 16))
    z_plus, z_minus = (lax.rem(r + 2, 8), c), (lax.rem(r + 6, 8), c)
    lo_mate = (r + 1 - 2 * x_lo, c)
    far_plus, far_minus = ((lax.rem(r + 2, 8) + 1 - 2 * x_lo, c), (lax.rem(r + 6, 8) + 1 - 2 * x_lo, c))

    barrier = pltpu.get_barrier_semaphore()
    mates = (core_mate, x_mate, y_plus, y_minus, z_plus, z_minus, lo_mate, far_plus, far_minus)
    for dev in mates:
        pl.semaphore_signal(barrier, inc=1, device_id=dev, device_id_type=MESH)

    def weight_copy(j, which):
        cols = pl.ds(pl.multiple_of(j * CW, CW), CW)
        src, dst = (gate_hbm, wg) if which == 0 else (up_hbm, wu)
        return pltpu.make_async_copy(src.at[:, cols], dst.at[:, cols], w_sem.at[which, j])

    def down_copy():
        return pltpu.make_async_copy(down_hbm, wd, w_sem.at[0, NJ])

    def loss_copy():
        return pltpu.make_async_copy(loss_hbm, loss, w_sem.at[1, NJ])

    def start_weights(j, _):
        weight_copy(j, 0).start()
        weight_copy(j, 1).start()
        return 0

    lax.fori_loop(0, NJ, start_weights, 0)
    loss_copy().start()

    own_rows = pl.multiple_of(r * 32, 32)
    stream_rows = pl.multiple_of(r * 16, 16)
    for h in range(2):
        lhs[1, h, pl.ds(stream_rows, 16), :] = tok_ref[h * 16 : (h + 1) * 16, :]
    for ref in (hid, back):
        ref[:, :, : 2 * CW] = jnp.zeros((2, HALF, 2 * CW), BF16)

    words = words_ref[...]
    parts = [lax.shift_right_logical(words, jnp.full_like(words, 8 * b)) & 255 for b in range(4)]
    octets = jnp.concatenate(parts, axis=0).astype(F32).astype(BF16)
    at = lax.broadcasted_iota(I32, (128, KD), 0)
    lane = lax.broadcasted_iota(I32, (128, KD), 1)
    pick = ((at % 32) * 4 + at // 32 == lane // 8).astype(F32).astype(BF16)
    spread = lax.dot_general(octets, pick, (((0,), (0,)), ((), ())), preferred_element_type=F32)
    bit = lax.broadcasted_iota(I32, (TOK, KD), 1) % 8
    signs = 2 * (lax.shift_right_logical(spread.astype(I32), bit) & 1) - 1
    signs = signs.astype(F32).astype(BF16)
    for i in range(TOK // 16):
        lhs[0, i % 2, i // 2 * 16 : (i // 2 + 1) * 16, :] = signs[i * 16 : (i + 1) * 16]

    pl.semaphore_wait(barrier, len(mates))

    def tok_region(k, at, rows, half):
        if half is None:
            return lhs.at[1, :, pl.ds(at, rows), :]
        return lhs.at[1, :, pl.ds(at, rows), pl.ds(half * (KD // 2), KD // 2)]

    def wide_region(ref, shift, width):
        def region(k, at, rows, half):
            end = (k - shift + 1) * GU * CW
            cols = pl.ds(pl.multiple_of(end - width, width), width)
            if half is None:
                return ref.at[:, pl.ds(at, rows), cols]
            return ref.at[pl.ds(half, 1), pl.ds(at, rows), cols]

        return region

    def cot_region(k, at, rows, half):
        h, n = k // 2, k % 2
        cols = pl.ds(pl.multiple_of(n * 2 * CW, 2 * CW), 2 * CW)
        if half is None:
            return cot.at[h, :, pl.ds(at, rows), cols]
        return cot.at[h, pl.ds(half, 1), pl.ds(at, rows), cols]

    z_axis = (z, z_plus, z_minus, lo_mate, far_plus, far_minus, x_lo)

    def along_z(region):
        return ShortSpread(*z_axis, 32, region, (s_send, s_recv))

    def along_y(region):
        return Spread(
            y, y_plus, y_minus, x_mate, x_hi, 16, core * 64, region, (g_send, g_recv), lambda k: lax.rem(k, NS)
        )

    tok_spread = along_z(tok_region)
    cot_spread = along_z(cot_region)
    hid_spread = [along_y(wide_region(hid, 0, w * CW)) for w in (GU // 2, GU)]
    back_spread = [along_y(wide_region(back, NG, w * CW)) for w in (GU // 2, GU)]
    log_code, bf_code = (log_encode, log_decode), (bf_encode, bf_decode)
    y_axis = (y, y_plus, y_minus, x_mate, x_hi)
    pre_rings = [None, Ring(
        *y_axis, 16, 8, log_code, (opp_s, opp_r, nb_s, nb_r, x_s, x_r, keep), (c_send, c_recv), log_code
    )]
    back_bufs = (opp_sb, opp_rb, nb_sb, nb_rb, x_sb, x_rb, keep)
    back_rings = [
        Ring(*y_axis, 16, n, bf_code, back_bufs, (c_send, c_recv), bf_code, base=GU * 2 - n) for n in (GU, GU * 2)
    ]
    row_bufs = (ropp_s, ropp_r, rnb_s, rnb_r, rx_s, rx_r, rkeep)
    last_bufs = (fopp_s, fopp_r, fnb_s, fnb_r, fx_s, fx_r, fkeep)
    row_ring = ShortRing(*z_axis, 32, 4, row_bufs, (r_send, r_recv))
    last_ring = ShortRing(*z_axis, 32, 2, last_bufs, (r_send, r_recv))

    tok_spread.first(NF)

    core_rows = pl.multiple_of(core * 64, 64)
    mate_rows = pl.multiple_of((1 - core) * 64, 64)
    share_rows = pl.ds(pl.multiple_of(core * 64 + y * 16 + x_hi * 8, 8), 8)

    def core_copy(k, ring):
        sl, part = lax.rem(k, NS), pl.ds(ring.base, ring.arrays)
        return rdma(
            res.at[sl, part, pl.ds(mate_rows, 64), :], d2d.at[sl, part], d_send.at[sl], d_recv.at[sl], core_mate
        )

    def wide_copy(spreader, k, rows):
        part = spreader.region(k, rows, 64, None)
        sl = spreader.slot(k)
        return rdma(part, part, g_send.at[sl, 4], g_recv.at[sl, 4], core_mate)

    def chip_term(k):
        sl = lax.rem(k, NS)

        def term(block, p):
            rows = pl.multiple_of(core_rows + block, 16)
            return res[sl, p, pl.ds(rows, 16), :] + d2d[sl, p, pl.ds(block, 16), :]

        return term

    def stage(t, lag, low, high, work):
        k = t - lag

        @pl.when((k >= low) & (k < high))
        def _():
            work(k)

    def sweep(low, high, shift, multiply, rings, spreaders, shares, accumulate, extra, after, early=0):
        def either(first, pair, k, work):
            if pair[0] is None:
                work(pair[1])
                return
            for small, one in ((True, pair[0]), (False, pair[1])):

                @pl.when((k == first) == small)
                def _():
                    work(one)

        def ring_stage(work):
            return lambda k: either(low, rings, k, lambda ring: work(k, ring))

        def spread_stage(work):
            return lambda k: either(high - NG, spreaders, k, lambda one: work(k - shift, one))

        def start_core(k, ring):
            core_copy(k, ring).start()

        def chip_add(k, ring):
            core_copy(k, ring).wait()
            ring.scatter(k, chip_term(k))

        def send_wide(k, one):
            one.last(k)
            wide_copy(one, k, core_rows).start()

        def wait_wide(k, one):
            wide_copy(one, k, core_rows).wait_send()
            wide_copy(one, k, mate_rows).wait_recv()

        start_cores = ring_stage(start_core)

        def begin(k):
            multiply(k)
            start_cores(k)

        chip_sum = ring_stage(chip_add)
        relay = ring_stage(lambda k, ring: ring.relay(k))
        gather_in = ring_stage(lambda k, ring: ring.gather_in(k))
        shared = ring_stage(lambda k, ring: shares(k, ring.finish(k), ring.base // 2))
        first = spread_stage(lambda k, one: one.first(k))
        second = spread_stage(lambda k, one: one.second(k))
        third = spread_stage(lambda k, one: one.third(k))
        to_mate = spread_stage(send_wide)
        from_mate = spread_stage(wait_wide)

        start = high - NG

        def step(t, _):
            if early:
                stage(t, LAG[2], low, low + 1, relay)
            stage(t, LAG[0], low, high, begin)
            if extra is not None:
                extra(t)
            stage(t, LAG[8], start, high, from_mate)
            stage(t, LAG[7], start, high, to_mate)
            stage(t, LAG[6], start, high, third)
            stage(t, LAG[5], start, high, second)
            stage(t, LAG[4], low, high, shared)
            stage(t, LAG[4], start, high, first)
            stage(t, LAG[3], low, high, gather_in)
            stage(t, LAG[2], low + early, high, relay)
            stage(t, LAG[1], low, high, chip_sum)
            stage(t, LAG[8], start, high, lambda k: accumulate(k - start))
            for work in after:
                work(t)
            return 0

        lax.fori_loop(low, high + LAG[8], step, 0)

    def cols_of(k):
        return pl.ds(pl.multiple_of(k * CW, CW), CW)

    def multiply_in(k):
        sl = lax.rem(k, NS)

        def probe_chunk(u):
            j = 2 * k + u
            weight_copy(j, 0).wait()
            weight_copy(j, 1).wait()
            left = lhs[0].reshape(TOK, KD)
            for p, weight in enumerate((wg, wu)):
                both = dot(left, weight[:, cols_of(j)])
                res[sl, 4 * u + p] = both[:HALF]
                res[sl, 4 * u + 2 + p] = both[HALF:]

        def token_unit(i):
            v = GU * k + i - 2 * NJ
            for p, weight in enumerate((wg, wu)):
                res[sl, 2 * i + p] = dot(lhs[1, v // NJ], weight[:, cols_of(v % NJ)])

        @pl.when(k <= NJ // 2)
        def _():
            probe_chunk(0)

        @pl.when(k < NJ // 2)
        def _():
            probe_chunk(1)

        @pl.when(k == NJ // 2)
        def _():
            tok_spread.last(NF)

        @pl.when(k > NJ // 2)
        def _():
            token_unit(0)
            token_unit(1)

        @pl.when(k >= NJ // 2)
        def _():
            token_unit(2)
            token_unit(3)

    def shares_in(k, sums, skip):
        for i in range(GU):
            n = GU * k + i
            v = n - 2 * NJ

            @pl.when(v < 0)
            def _():
                at = n % 2 * NJ + n // 2
                pre[at, 0] = sums[2 * i]
                pre[at, 1] = sums[2 * i + 1]

            @pl.when(v >= 0)
            def _():
                pre[n, 0] = sums[2 * i]
                pre[n, 1] = sums[2 * i + 1]
                active, slopes, _ = silu_parts(pre[n, 0])
                up_pre, gate_tan, up_tan = pre[n, 1], pre[v, 0], pre[v, 1]
                hid[0, share_rows, cols_of(v + 2)] = (active * up_pre).astype(BF16)
                hid[1, share_rows, cols_of(v + 2)] = (slopes * gate_tan * up_pre + active * up_tan).astype(BF16)

    def loss_of_tokens():
        loss_copy().wait()
        lanes = lax.broadcasted_iota(I32, (1, 128), 1)

        for i in range(32):
            tid = ids_ref[own_rows + i]
            line = loss[pl.ds(tid // 128, 1), :]
            value = jnp.sum(jnp.where(lanes == tid % 128, line, 0.0), axis=1, keepdims=True)
            scale[i : i + 1, :] = jnp.broadcast_to(value, (1, 128))

    def token_spread(t):
        @pl.when(t == 3)
        def _():
            tok_spread.third(NF)

    def token_steps(t):
        @pl.when(t == 5)
        def _():
            down_copy().start()

        @pl.when(t == 8)
        def _():
            loss_of_tokens()

        @pl.when(t == NJ)
        def _():
            down_copy().wait()

    def gather_out(g):
        @pl.when(g == 0)
        def _():
            add_out(0, 2, 0, 2, True)

        @pl.when((g == 1) | (g == 2))
        def _():
            add_out(0, GU * g, GU * g - 2, GU, False)

        @pl.when(g == 3)
        def _():
            add_out(0, GU * 3, GU * 3 - 2, 3, False)
            add_out(1, GU * 3 + 3, 0, 1, True)

        @pl.when(g > 3)
        def _():
            add_out(1, GU * g, GU * g - 2 - NJ, GU, False)

    def gather_last(g):
        @pl.when(g == 3)
        def _():
            add_last(0, 1, True, pl.ds(0, KD))

        @pl.when((g > 3) & (g < NG - 1))
        def _():
            add_last(GU * g - 2 - NJ, GU, False, pl.ds(0, KD))

    def slices(first, j, units):
        width = units * CW
        return pl.ds(pl.multiple_of(first * CW, CW), width), pl.ds(pl.multiple_of(j * CW, CW), width)

    def add_out(h, first, j, units, opens):
        at, unit = slices(first, j, units)
        part = dot(hid[:, :, at].reshape(2 * HALF, units * CW), wd[unit, :])
        acc[h] = part if opens else acc[h] + part

    def add_last(j, units, opens, cols):
        part = 0.0
        for q, weight in enumerate((wg, wu)):
            at, unit = slices(j + 2, j, units)
            later, _ = slices(j + 2 + NJ, j, units)
            left = jnp.concatenate([back[q, :, at], back[q, :, later]], axis=0)
            part = part + dot_t(left, weight[cols, unit])
        last[:, cols] = part if opens else last[:, cols] + part

    def out_term(e):
        h, n = e // 2, e % 2

        def term(block, i):
            at = (2 * n + i // 2) * CW
            return acc[h, pl.ds(pl.multiple_of(i % 2 * HALF + block, 32), 32), at : at + CW]

        return term

    def cotangents(e):
        h, n = e // 2, e % 2
        sums = row_ring.finish(e)
        weight = scale[h * 16 : (h + 1) * 16, :1]
        rows = pl.ds(stream_rows, 16)
        for i in range(2):
            cols = cols_of(2 * n + i)
            tan = weight * (lhs[0, h, rows, cols].astype(F32) + sums[2 * i + 1])
            tan_ref[h * 16 : (h + 1) * 16, cols] = tan
            cot[h, 0, rows, cols] = (weight * (lhs[1, h, rows, cols].astype(F32) + sums[2 * i])).astype(BF16)
            cot[h, 1, rows, cols] = tan.astype(BF16)
        cot_spread.first(e)

    row_works = dict(
        S=lambda e: row_ring.scatter(e, out_term(e)),
        R=row_ring.relay,
        F=cotangents,
        T=cot_spread.third,
        L=cot_spread.last,
    )

    def in_order(works, names):
        for name in names.split():
            works[name[0]](int(name[1]))

    def at_steps(works, table):
        def steps(t):
            for step, names in table:

                @pl.when(t == step)
                def _():
                    in_order(works, names)

        return steps

    done = NJ - 4 + LAG[8]
    sweep(
        0, NJ, NJ - NG, multiply_in, pre_rings, hid_spread, shares_in, gather_out, token_steps,
        (token_spread, at_steps(row_works, ((done, "S0 S1"), (done + 2, "R0 R1"), (done + 3, "S2 S3")))),
    )
    in_order(row_works, "F0 F1 R2 R3 T0 T1 F2 L0 F3 L1")

    def multiply_back(k):
        @pl.when(k == NJ + 3)
        def _():
            cot_spread.last(2)
            cot_spread.last(3)

        sl = lax.rem(k, NS)
        for i in range(GU):
            v = jnp.maximum(GU * (k - NJ) - 2 + i, 0)
            left = cot[v // NJ].reshape(TOK, KD)
            both = dot_t(left, wd[pl.ds(pl.multiple_of(v % NJ * CW, CW), CW), :])
            res[sl, 2 * i] = both[:HALF]
            res[sl, 2 * i + 1] = both[HALF:]

    def shares_back(k, sums, skip):
        for i in range(skip, GU):
            v = GU * (k - NJ) - 2 + i
            backward, back_tan = sums[2 * (i - skip)], sums[2 * (i - skip) + 1]

            @pl.when(v >= 0)
            def _():
                active, slopes, curves = silu_parts(pre[2 * NJ + v, 0])
                up_pre, gate_tan, up_tan = pre[2 * NJ + v, 1], pre[v, 0], pre[v, 1]
                gate_back = (
                    back_tan * up_pre * slopes
                    + backward * up_tan * slopes
                    + backward * up_pre * curves * gate_tan
                )
                up_back = back_tan * active + backward * slopes * gate_tan
                back[0, share_rows, cols_of(v + 2)] = gate_back.astype(BF16)
                back[1, share_rows, cols_of(v + 2)] = up_back.astype(BF16)

    def last_term(f):
        h, n = f // 2, f % 2

        def term(block, i):
            at = (2 * n + i) * CW
            return last[pl.ds(pl.multiple_of(h * HALF + block, 32), 32), at : at + CW]

        return term

    def finish_last(f):
        h, n = f // 2, f % 2
        sums = last_ring.finish(f)
        for i in range(2):
            at = (2 * n + i) * CW
            out_ref[h * 16 : (h + 1) * 16, at : at + CW] = sums[i]

    last_works = dict(
        S=lambda f: last_ring.scatter(f, last_term(f)),
        R=last_ring.relay,
        F=finish_last,
    )

    sweep(
        NJ, NJ + NG, NJ - NG, multiply_back, back_rings, back_spread, shares_back, gather_last,
        None, (at_steps(row_works, ((NJ + 1, "T2"), (NJ + 2, "T3"))),), 1,
    )
    for n in range(2):
        add_last(GU * (NG - 1) - 2 - NJ, GU, False, pl.ds(n * KD // 2, KD // 2))
        in_order(last_works, f"S{n} S{n + 2}")
    in_order(last_works, "R0 R2 R1 R3 F0 F2 F1 F3")


def ring_buffers(arrays, rows, width, dtype, x_dtype):
    half = rows // 2
    shapes = ((arrays, rows), (arrays, rows), (2, arrays, rows), (2, arrays, rows))
    return [pltpu.VMEM((NS, *shape, width), dtype) for shape in shapes] + [
        pltpu.VMEM((NS, arrays, half, width), x_dtype) for _ in range(2)
    ]


def short_buffers(arrays, rows, width):
    half = rows // 2
    shapes = ((arrays, rows), (arrays, rows), (2, arrays, rows), (2, 2, arrays, half), (arrays, half), (arrays, half))
    return [pltpu.VMEM((NS, *shape, width), BF16) for shape in shapes]


def block(tokens, words, token_ids, loss_weight, gate_weight, up_weight, down_weight):
    vmem = lambda shape, dtype: pltpu.VMEM(shape, dtype)
    sem = lambda *shape: pltpu.SemaphoreType.DMA(shape)
    anywhere = pl.BlockSpec(memory_space=pl.ANY)
    inside = pl.BlockSpec(memory_space=pltpu.VMEM)
    scalars = pl.BlockSpec(memory_space=pltpu.SMEM)
    return pl.pallas_call(
        block_kernel,
        out_shape=[jax.ShapeDtypeStruct((32, KD), F32)] * 2,
        in_specs=[inside, inside, scalars, anywhere, anywhere, anywhere, anywhere],
        out_specs=[inside, inside],
        scratch_shapes=[
            vmem((KD, HW), BF16),
            vmem((KD, HW), BF16),
            vmem((HW, KD), BF16),
            vmem(loss_weight.shape, F32),
            vmem((32, 128), F32),
            vmem((2, 2, HALF, KD), BF16),
            vmem((2, 2, HALF, KD), BF16),
            vmem((2, HALF, WIN), BF16),
            vmem((2, HALF, WIN), BF16),
            vmem((NS, 8, HALF, CW), F32),
            vmem((NS, 8, HALF // 2, CW), F32),
            vmem((NK, 16, 16, CW), F32),
            *ring_buffers(8, 16, CW, I16, I16),
            *ring_buffers(8, 16, CW, BF16, BF16),
            vmem((4 * NJ, 2, 8, CW), F32),
            vmem((NS, 8, 32, CW), F32),
            *short_buffers(4, 32, CW),
            vmem((NS, 4, 32, CW), F32),
            *short_buffers(2, 32, CW),
            vmem((2, TOK, KD), F32),
            vmem((TOK, KD), F32),
            sem(2, NJ + 1),
            sem(NS),
            sem(NS),
            sem(NS, 4),
            sem(NS, 4),
            sem(NS, 5),
            sem(NS, 5),
            sem(NS, 4),
            sem(NS, 4),
            sem(NF + 1, 2),
            sem(NF + 1, 6),
        ],
        compiler_params=pltpu.CompilerParams(
            collective_id=0, has_side_effects=True, vmem_limit_bytes=67043328
        ),
    )(tokens, words, token_ids, loss_weight, gate_weight, up_weight, down_weight)


def on_device(tokens, probe_words, token_ids, loss_weight, gate_weight, up_weight, down_weight):
    tan, summed = block(
        tokens, probe_words.T, token_ids, loss_weight.reshape(-1, 128), gate_weight, up_weight, down_weight
    )
    return tan + summed


def solution(mesh):
    return jax.shard_map(
        on_device,
        mesh=mesh,
        in_specs=(
            P("row", "col"),
            P(None, "col"),
            P(),
            P(),
            P("col", "row"),
            P("col", "row"),
            P("row", "col"),
        ),
        out_specs=P("row", "col"),
        check_vma=False,
    )
```

```python
import functools
import math

import jax
import jax.numpy as jnp
from jax import lax
from jax.experimental import pallas as pl
from jax.experimental.pallas import tpu as pltpu
from jax.sharding import PartitionSpec as P

MESH = pl.DeviceIdType.MESH
F32, BF16, I16, I32 = jnp.float32, jnp.bfloat16, jnp.int16, jnp.int32

TOK = 256
HALF = 128
KD = 1024
HW = 3328
CW = 256
NJ = HW // CW
NF = KD // CW
GU = 4
NG = (2 * NJ + 2) // GU
WIN = NG * GU * CW
LAG = (0, 1, 3, 5, 7, 9, 11, 13, 14)
NS = 4
NK = 8

CODE_UNIT = 1024.0
CODE_SCALE = 32700.0 / math.log1p(4700.0 * CODE_UNIT)


def log_encode(x):
    mag = jnp.log(1.0 + jnp.abs(x) * CODE_UNIT) * CODE_SCALE
    q = (mag + 0.5).astype(I32)
    return jnp.where(x < 0, -q, q).astype(I16)


def log_decode(y):
    y = y.astype(I32).astype(F32)
    mag = (jnp.exp(jnp.abs(y) * (1.0 / CODE_SCALE)) - 1.0) * (1.0 / CODE_UNIT)
    return jnp.where(y < 0, -mag, mag)


def bf_encode(x):
    return x.astype(BF16)


def bf_decode(x):
    return x.astype(F32)


def dot(a, b):
    return jnp.dot(a, b, preferred_element_type=F32)


def dot_t(a, b):
    return lax.dot_general(a, b, (((1,), (1,)), ((), ())), preferred_element_type=F32)


def silu_parts(pre_act):
    sig = 1.0 / (1.0 + jnp.exp(-pre_act))
    active = pre_act * sig
    slopes = sig * (1.0 + pre_act * (1.0 - sig))
    curves = sig * (1.0 - sig) * (2.0 + pre_act * (1.0 - 2.0 * sig))
    return active, slopes, curves


def rdma(src, dst, ssem, rsem, dev):
    return pltpu.make_async_remote_copy(
        src_ref=src, dst_ref=dst, send_sem=ssem, recv_sem=rsem, device_id=dev, device_id_type=MESH
    )


class Ring:
    def __init__(self, pos, plus, minus, mate, side, rows, arrays, code, bufs, sems, x_code, base=0):
        self.pos, self.plus, self.minus, self.mate, self.side = pos, plus, minus, mate, side
        self.rows, self.half = rows, rows // 2
        self.arrays, self.each, self.base, self.own = arrays, arrays // 2, base, arrays + base
        self.enc, self.dec = code
        self.x_enc, self.x_dec = x_code
        self.opp_s, self.opp_r, self.nb_s, self.nb_r, self.x_s, self.x_r, self.keep = bufs
        self.ss, self.rs = sems

    def block(self, delta):
        return pl.multiple_of(lax.rem(self.pos + (4 + delta), 4) * self.rows, self.rows)

    def opp_copy(self, k, d):
        dev = self.plus if d == 0 else self.minus
        sl, part = lax.rem(k, NS), pl.ds(self.base + d * self.each, self.each)
        return rdma(self.opp_s.at[sl, part], self.opp_r.at[sl, part], self.ss.at[sl, d], self.rs.at[sl, d], dev)

    def nb_copy(self, k, d):
        dev = self.plus if d == 0 else self.minus
        sl, part = lax.rem(k, NS), pl.ds(self.base, self.arrays)
        return rdma(
            self.nb_s.at[sl, d, part], self.nb_r.at[sl, d, part], self.ss.at[sl, 2], self.rs.at[sl, 2], dev
        )

    def nb_wait(self, k):
        sl, part = lax.rem(k, NS), pl.ds(self.base, self.arrays)
        ref = self.nb_r.at[sl, :, part]
        rdma(ref, ref, self.ss.at[sl, 2], self.rs.at[sl, 2], self.plus).wait()

    def x_copy(self, k):
        sl, part = lax.rem(k, NS), pl.ds(self.base, self.arrays)
        return rdma(self.x_s.at[sl, part], self.x_r.at[sl, part], self.ss.at[sl, 3], self.rs.at[sl, 3], self.mate)

    def of(self, d):
        return range(self.base + d * self.each, self.base + (d + 1) * self.each)

    def scatter(self, k, term):
        sl, kp = lax.rem(k, NS), lax.rem(k, NK)
        for d in range(2):
            for i in self.of(d):
                self.opp_s[sl, i] = self.enc(term(self.block(2), i))
            self.opp_copy(k, d).start()
        for d in range(2):
            near, far = (1, -1) if d == 0 else (-1, 1)
            for i in self.of(d):
                self.keep[kp, i] = term(self.block(near), i)
                self.nb_s[sl, 1 - d, i] = self.enc(term(self.block(far), i))
                self.keep[kp, self.own + i] = term(self.block(0), i)

    def relay(self, k):
        sl, kp = lax.rem(k, NS), lax.rem(k, NK)
        for d in range(2):
            self.opp_copy(k, d).wait()
            for i in self.of(d):
                self.nb_s[sl, d, i] = self.enc(self.keep[kp, i] + self.dec(self.opp_r[sl, i]))
            self.nb_copy(k, d).start()

    def gather_in(self, k):
        sl, kp = lax.rem(k, NS), lax.rem(k, NK)
        self.nb_wait(k)
        other = pl.multiple_of((1 - self.side) * self.half, self.half)
        for i in range(self.base, self.own):
            own = self.own + i
            self.keep[kp, own] += self.dec(self.nb_r[sl, 0, i]) + self.dec(self.nb_r[sl, 1, i])
            self.x_s[sl, i] = self.x_enc(self.keep[kp, own, pl.ds(other, self.half), :])
        self.x_copy(k).start()

    def finish(self, k):
        sl, kp = lax.rem(k, NS), lax.rem(k, NK)
        self.x_copy(k).wait()
        own = pl.multiple_of(self.side * self.half, self.half)
        return [
            self.keep[kp, self.own + i, pl.ds(own, self.half), :] + self.x_dec(self.x_r[sl, i])
            for i in range(self.base, self.own)
        ]


class Spread:
    def __init__(self, pos, plus, minus, mate, side, rows, base, region, sems, slot):
        self.pos, self.plus, self.minus, self.mate, self.side = pos, plus, minus, mate, side
        self.rows, self.half, self.base, self.region = rows, rows // 2, base, region
        self.ss, self.rs = sems
        self.slot = slot

    def start_of(self, delta):
        return pl.multiple_of(self.base + lax.rem(self.pos + (4 + delta), 4) * self.rows, self.rows)

    def copy(self, k, i, ref, dev):
        sl = self.slot(k)
        return rdma(ref, ref, self.ss.at[sl, i], self.rs.at[sl, i], dev)

    def mine(self, k):
        at = pl.multiple_of(self.start_of(0) + self.side * self.half, self.half)
        return self.copy(k, 0, self.region(k, at, self.half, None), self.mate)

    def first(self, k):
        self.mine(k).start()

    def second(self, k):
        self.mine(k).wait_send()
        at = pl.multiple_of(self.start_of(0) + (1 - self.side) * self.half, self.half)
        self.copy(k, 0, self.region(k, at, self.half, None), self.mate).wait_recv()
        ref = self.region(k, self.start_of(0), self.rows, None)
        self.copy(k, 1, ref, self.plus).start()
        self.copy(k, 2, ref, self.minus).start()

    def third(self, k):
        ref = self.region(k, self.start_of(0), self.rows, None)
        self.copy(k, 1, ref, self.plus).wait_send()
        self.copy(k, 2, ref, self.minus).wait_send()
        self.copy(k, 1, self.region(k, self.start_of(-1), self.rows, None), self.plus).wait_recv()
        self.copy(k, 3, self.region(k, self.start_of(-1), self.rows, 0), self.plus).start()
        self.copy(k, 2, self.region(k, self.start_of(1), self.rows, None), self.minus).wait_recv()
        self.copy(k, 3, self.region(k, self.start_of(1), self.rows, 1), self.minus).start()

    def last(self, k):
        self.copy(k, 3, self.region(k, self.start_of(2), self.rows, None), self.plus).wait()


class ShortRing:
    def __init__(self, pos, plus, minus, mate, far_plus, far_minus, side, rows, arrays, bufs, sems):
        self.pos, self.mate, self.side = pos, mate, side
        self.near, self.far = (plus, minus), (far_plus, far_minus)
        self.rows, self.half = rows, rows // 2
        self.arrays, self.each = arrays, arrays // 2
        self.opp_s, self.opp_r, self.nb_s, self.nb_r, self.x_s, self.x_r, self.keep = bufs
        self.ss, self.rs = sems

    def block(self, delta):
        return pl.multiple_of(lax.rem(self.pos + (4 + delta), 4) * self.rows, self.rows)

    def side_rows(self, other):
        side = 1 - self.side if other else self.side
        return pl.ds(pl.multiple_of(side * self.half, self.half), self.half)

    def opp_copy(self, k, d):
        sl, part = k % NS, pl.ds(d * self.each, self.each)
        return rdma(
            self.opp_s.at[sl, part], self.opp_r.at[sl, part], self.ss.at[sl, d], self.rs.at[sl, d], self.near[d]
        )

    def nb_copy(self, k, d, other):
        sl = k % NS
        dev = self.far[d] if other else self.near[d]
        src = self.nb_s.at[sl, d, :, self.side_rows(other), :]
        return rdma(src, self.nb_r.at[sl, d, other], self.ss.at[sl, 2], self.rs.at[sl, 2], dev)

    def nb_wait(self, k):
        sl = k % NS
        rdma(self.nb_r.at[sl], self.nb_r.at[sl], self.ss.at[sl, 2], self.rs.at[sl, 2], self.mate).wait()

    def x_copy(self, k):
        sl = k % NS
        return rdma(self.x_s.at[sl], self.x_r.at[sl], self.ss.at[sl, 3], self.rs.at[sl, 3], self.mate)

    def of(self, d):
        return range(d * self.each, (d + 1) * self.each)

    def scatter(self, k, term):
        sl = k % NS
        for d in range(2):
            for i in self.of(d):
                self.opp_s[sl, i] = bf_encode(term(self.block(2), i))
            self.opp_copy(k, d).start()
        for d in range(2):
            near, far = (1, -1) if d == 0 else (-1, 1)
            for i in self.of(d):
                self.keep[sl, i] = term(self.block(near), i)
                self.nb_s[sl, 1 - d, i] = bf_encode(term(self.block(far), i))
                self.keep[sl, self.arrays + i] = term(self.block(0), i)
                self.x_s[sl, i] = bf_encode(self.keep[sl, self.arrays + i, self.side_rows(1), :])
        self.x_copy(k).start()

    def relay(self, k):
        sl = k % NS
        for d in range(2):
            self.opp_copy(k, d).wait()
            for i in self.of(d):
                self.nb_s[sl, d, i] = bf_encode(self.keep[sl, i] + bf_decode(self.opp_r[sl, i]))
            for other in (1, 0):
                self.nb_copy(k, d, other).start()

    def finish(self, k):
        sl = k % NS
        self.x_copy(k).wait()
        self.nb_wait(k)
        sums = []
        for i in range(self.arrays):
            total = self.keep[sl, self.arrays + i, self.side_rows(0), :] + bf_decode(self.x_r[sl, i])
            for d in range(2):
                for other in range(2):
                    total = total + bf_decode(self.nb_r[sl, d, other, i])
            sums.append(total)
        return sums


class ShortSpread:
    def __init__(self, pos, plus, minus, mate, far_plus, far_minus, side, rows, region, sems):
        self.pos, self.side, self.rows, self.half, self.region = pos, side, rows, rows // 2, region
        self.near, self.far, self.mate = (plus, minus), (far_plus, far_minus), mate
        self.ss, self.rs = sems

    def start_of(self, delta):
        return pl.multiple_of(lax.rem(self.pos + (4 + delta), 4) * self.rows, self.rows)

    def part(self, k, delta, other):
        side = 1 - self.side if other else self.side
        return self.region(k, pl.multiple_of(self.start_of(delta) + side * self.half, self.half), self.half, None)

    def copy(self, k, i, ref, dev):
        return rdma(ref, ref, self.ss.at[k, i // 5], self.rs.at[k, i], dev)

    def own_copies(self, k):
        mine = self.part(k, 0, 0)
        far = [self.copy(k, 3 + d, mine, self.far[d]) for d in range(2)]
        near = [self.copy(k, 1 + d, mine, self.near[d]) for d in range(2)]
        return far + near + [self.copy(k, 0, mine, self.mate)]

    def relay_copy(self, k, d):
        return self.copy(k, 5, self.region(k, self.start_of(2 * d - 1), self.rows, d), self.near[d])

    def first(self, k):
        for one in self.own_copies(k):
            one.start()

    def third(self, k):
        for d in range(2):
            self.copy(k, 1 + d, self.part(k, 2 * d - 1, 0), self.near[d]).wait_recv()
            self.copy(k, 3 + d, self.part(k, 2 * d - 1, 1), self.far[d]).wait_recv()
            self.relay_copy(k, d).start()

    def last(self, k):
        self.copy(k, 0, self.region(k, 0, 5 * self.half, None), self.mate).wait_send()
        self.copy(k, 0, self.part(k, 0, 1), self.mate).wait_recv()
        self.copy(k, 5, self.region(k, self.start_of(2), self.rows, None), self.mate).wait()


def block_kernel(
    tok_ref,
    words_ref,
    ids_ref,
    loss_hbm,
    gate_hbm,
    up_hbm,
    down_hbm,
    out_ref,
    w_in,
    wd,
    loss,
    scale,
    lhs,
    cot,
    hid,
    back,
    res,
    d2d,
    keep,
    opp_s,
    opp_r,
    nb_s,
    nb_r,
    x_s,
    x_r,
    opp_sb,
    opp_rb,
    nb_sb,
    nb_rb,
    x_sb,
    x_rb,
    pre,
    rkeep,
    ropp_s,
    ropp_r,
    rnb_s,
    rnb_r,
    rx_s,
    rx_r,
    fkeep,
    fopp_s,
    fopp_r,
    fnb_s,
    fnb_r,
    fx_s,
    fx_r,
    acc,
    last,
    own_tan,
    w_sem,
    d_send,
    d_recv,
    c_send,
    c_recv,
    g_send,
    g_recv,
    r_send,
    r_recv,
    s_send,
    s_recv,
):
    r, c = lax.axis_index("row"), lax.axis_index("col")
    z, x_lo = r // 2, r % 2
    y, x_hi, core = c // 4, (c // 2) % 2, c % 2
    core_mate = (r, c + 1 - 2 * core)
    x_mate = (r, c + 2 - 4 * x_hi)
    y_plus, y_minus = (r, lax.rem(c + 4, 16)), (r, lax.rem(c + 12, 16))
    z_plus, z_minus = (lax.rem(r + 2, 8), c), (lax.rem(r + 6, 8), c)
    lo_mate = (r + 1 - 2 * x_lo, c)
    far_plus, far_minus = ((lax.rem(r + 2, 8) + 1 - 2 * x_lo, c), (lax.rem(r + 6, 8) + 1 - 2 * x_lo, c))

    barrier = pltpu.get_barrier_semaphore()
    mates = (core_mate, x_mate, y_plus, y_minus, z_plus, z_minus, lo_mate, far_plus, far_minus)
    for dev in mates:
        pl.semaphore_signal(barrier, inc=1, device_id=dev, device_id_type=MESH)

    wg, wu = w_in.at[0], w_in.at[1]

    def weight_wait(j):
        part = w_in.at[:, :, pl.ds(pl.multiple_of(j * CW, CW), CW)]
        pltpu.make_async_copy(part, part, w_sem.at[0, j]).wait()

    def weight_copy(j, which):
        cols = pl.ds(pl.multiple_of(j * CW, CW), CW)
        src, dst = (gate_hbm, wg) if which == 0 else (up_hbm, wu)
        return pltpu.make_async_copy(src.at[:, cols], dst.at[:, cols], w_sem.at[0, j])

    def down_copy():
        return pltpu.make_async_copy(down_hbm, wd, w_sem.at[0, NJ])

    def loss_copy():
        return pltpu.make_async_copy(loss_hbm, loss, w_sem.at[0, NJ + 1])

    def start_weights(j, _):
        weight_copy(j, 0).start()
        weight_copy(j, 1).start()
        return 0

    lax.fori_loop(0, NJ, start_weights, 0)
    loss_copy().start()

    own_rows = pl.multiple_of(r * 32, 32)
    stream_rows = pl.multiple_of(r * 16, 16)
    for h in range(2):
        lhs[1, h, pl.ds(stream_rows, 16), :] = tok_ref[h * 16 : (h + 1) * 16, :]
    for ref in (hid, back):
        ref[:, :, : 2 * CW] = jnp.zeros((2, HALF, 2 * CW), BF16)

    words = words_ref[...]
    parts = [lax.shift_right_logical(words, jnp.full_like(words, 8 * b)) & 255 for b in range(4)]
    octets = jnp.concatenate(parts, axis=0).astype(F32).astype(BF16)
    at = lax.broadcasted_iota(I32, (128, KD), 0)
    lane = lax.broadcasted_iota(I32, (128, KD), 1)
    pick = ((at % 32) * 4 + at // 32 == lane // 8).astype(F32).astype(BF16)
    spread = lax.dot_general(octets, pick, (((0,), (0,)), ((), ())), preferred_element_type=F32)
    bit = lax.broadcasted_iota(I32, (TOK, KD), 1) % 8
    signs = 2 * (lax.shift_right_logical(spread.astype(I32), bit) & 1) - 1
    signs = signs.astype(F32).astype(BF16)
    for i in range(TOK // 16):
        lhs[0, i % 2, i // 2 * 16 : (i // 2 + 1) * 16, :] = signs[i * 16 : (i + 1) * 16]

    pl.semaphore_wait(barrier, len(mates))

    def tok_region(k, at, rows, half):
        if half is None:
            return lhs.at[1, :, pl.ds(at, rows), :]
        return lhs.at[1, :, pl.ds(at, rows), pl.ds(half * (KD // 2), KD // 2)]

    def wide_region(ref, shift, width):
        def region(k, at, rows, half):
            end = (k - shift + 1) * GU * CW
            cols = pl.ds(pl.multiple_of(end - width, width), width)
            if half is None:
                return ref.at[:, pl.ds(at, rows), cols]
            return ref.at[pl.ds(half, 1), pl.ds(at, rows), cols]

        return region

    def cot_region(k, at, rows, half):
        h, n = k // 2, k % 2
        cols = pl.ds(pl.multiple_of(n * 2 * CW, 2 * CW), 2 * CW)
        if half is None:
            return cot.at[h, :, pl.ds(at, rows), cols]
        return cot.at[h, pl.ds(half, 1), pl.ds(at, rows), cols]

    z_axis = (z, z_plus, z_minus, lo_mate, far_plus, far_minus, x_lo)

    def along_z(region):
        return ShortSpread(*z_axis, 32, region, (s_send, s_recv))

    def along_y(region):
        return Spread(
            y, y_plus, y_minus, x_mate, x_hi, 16, core * 64, region, (g_send, g_recv), lambda k: lax.rem(k, NS)
        )

    tok_spread = along_z(tok_region)
    cot_spread = along_z(cot_region)
    hid_spread = [along_y(wide_region(hid, 0, w * CW)) for w in (GU // 2, GU)]
    back_spread = [along_y(wide_region(back, NG, w * CW)) for w in (GU // 2, GU)]
    log_code, bf_code = (log_encode, log_decode), (bf_encode, bf_decode)
    y_axis = (y, y_plus, y_minus, x_mate, x_hi)
    pre_rings = [None, Ring(
        *y_axis, 16, 8, log_code, (opp_s, opp_r, nb_s, nb_r, x_s, x_r, keep), (c_send, c_recv), log_code
    )]
    back_bufs = (opp_sb, opp_rb, nb_sb, nb_rb, x_sb, x_rb, keep)
    back_rings = [
        Ring(*y_axis, 16, n, bf_code, back_bufs, (c_send, c_recv), bf_code, base=GU * 2 - n) for n in (GU, GU * 2)
    ]
    row_bufs = (ropp_s, ropp_r, rnb_s, rnb_r, rx_s, rx_r, rkeep)
    last_bufs = (fopp_s, fopp_r, fnb_s, fnb_r, fx_s, fx_r, fkeep)
    row_ring = ShortRing(*z_axis, 32, 4, row_bufs, (r_send, r_recv))
    last_ring = ShortRing(*z_axis, 32, 2, last_bufs, (r_send, r_recv))

    tok_spread.first(NF)

    core_rows = pl.multiple_of(core * 64, 64)
    mate_rows = pl.multiple_of((1 - core) * 64, 64)
    share_rows = pl.ds(pl.multiple_of(core * 64 + y * 16 + x_hi * 8, 8), 8)

    def core_copy(k, ring):
        sl, part = lax.rem(k, NS), pl.ds(ring.base, ring.arrays)
        return rdma(
            res.at[sl, part, pl.ds(mate_rows, 64), :], d2d.at[sl, part], d_send.at[sl], d_recv.at[sl], core_mate
        )

    def wide_copy(spreader, k, rows):
        part = spreader.region(k, rows, 64, None)
        sl = spreader.slot(k)
        return rdma(part, part, g_send.at[sl, 4], g_recv.at[sl, 4], core_mate)

    def chip_term(k):
        sl = lax.rem(k, NS)

        def term(block, p):
            rows = pl.multiple_of(core_rows + block, 16)
            return res[sl, p, pl.ds(rows, 16), :] + d2d[sl, p, pl.ds(block, 16), :]

        return term

    def stage(t, lag, low, high, work):
        k = t - lag

        @pl.when((k >= low) & (k < high))
        def _():
            work(k)

    def sweep(low, high, shift, multiply, rings, spreaders, shares, accumulate, extra, after, early=0):
        def either(first, pair, k, work):
            if pair[0] is None:
                work(pair[1])
                return
            for small, one in ((True, pair[0]), (False, pair[1])):

                @pl.when((k == first) == small)
                def _():
                    work(one)

        def ring_stage(work):
            return lambda k: either(low, rings, k, lambda ring: work(k, ring))

        def spread_stage(work):
            return lambda k: either(high - NG, spreaders, k, lambda one: work(k - shift, one))

        def start_core(k, ring):
            core_copy(k, ring).start()

        def chip_add(k, ring):
            core_copy(k, ring).wait()
            ring.scatter(k, chip_term(k))

        def send_wide(k, one):
            one.last(k)
            wide_copy(one, k, core_rows).start()

        def wait_wide(k, one):
            wide_copy(one, k, core_rows).wait_send()
            wide_copy(one, k, mate_rows).wait_recv()

        start_cores = ring_stage(start_core)

        def begin(k):
            multiply(k)
            start_cores(k)

        chip_sum = ring_stage(chip_add)
        relay = ring_stage(lambda k, ring: ring.relay(k))
        gather_in = ring_stage(lambda k, ring: ring.gather_in(k))
        shared = ring_stage(lambda k, ring: shares(k, ring.finish(k), ring.base // 2))
        first = spread_stage(lambda k, one: one.first(k))
        second = spread_stage(lambda k, one: one.second(k))
        third = spread_stage(lambda k, one: one.third(k))
        to_mate = spread_stage(send_wide)
        from_mate = spread_stage(wait_wide)

        start = high - NG

        def step(t, _):
            if early:
                stage(t, LAG[2], low, low + 1, relay)
            stage(t, LAG[0], low, high, begin)
            if extra is not None:
                extra(t)
            stage(t, LAG[8], start, high, from_mate)
            stage(t, LAG[7], start, high, to_mate)
            stage(t, LAG[6], start, high, third)
            stage(t, LAG[5], start, high, second)
            stage(t, LAG[4], low, high, shared)
            stage(t, LAG[4], start, high, first)
            stage(t, LAG[3], low, high, gather_in)
            stage(t, LAG[2], low + early, high, relay)
            stage(t, LAG[1], low, high, chip_sum)
            stage(t, LAG[8], start, high, lambda k: accumulate(k - start))
            for work in after:
                work(t)
            return 0

        lax.fori_loop(low, high + LAG[8], step, 0)

    def cols_of(k):
        return pl.ds(pl.multiple_of(k * CW, CW), CW)

    def multiply_in(k):
        sl = lax.rem(k, NS)

        def probe_chunk(u):
            j = 2 * k + u
            weight_wait(j)
            left = lhs[0].reshape(TOK, KD)
            for p, weight in enumerate((wg, wu)):
                both = dot(left, weight[:, cols_of(j)])
                res[sl, 4 * u + p] = both[:HALF]
                res[sl, 4 * u + 2 + p] = both[HALF:]

        def token_unit(i):
            v = GU * k + i - 2 * NJ
            for p, weight in enumerate((wg, wu)):
                res[sl, 2 * i + p] = dot(lhs[1, v // NJ], weight[:, cols_of(v % NJ)])

        @pl.when(k <= NJ // 2)
        def _():
            probe_chunk(0)

        @pl.when(k < NJ // 2)
        def _():
            probe_chunk(1)

        @pl.when(k == NJ // 2)
        def _():
            tok_spread.last(NF)

        @pl.when(k > NJ // 2)
        def _():
            token_unit(0)
            token_unit(1)

        @pl.when(k >= NJ // 2)
        def _():
            token_unit(2)
            token_unit(3)

    def shares_in(k, sums, skip):
        for i in range(GU):
            n = GU * k + i
            v = n - 2 * NJ

            @pl.when(v < 0)
            def _():
                at = n % 2 * NJ + n // 2
                pre[at, 0] = sums[2 * i]
                pre[at, 1] = sums[2 * i + 1]

            @pl.when(v >= 0)
            def _():
                pre[n, 0] = sums[2 * i]
                pre[n, 1] = sums[2 * i + 1]
                active, slopes, _ = silu_parts(pre[n, 0])
                up_pre, gate_tan, up_tan = pre[n, 1], pre[v, 0], pre[v, 1]
                hid[0, share_rows, cols_of(v + 2)] = (active * up_pre).astype(BF16)
                hid[1, share_rows, cols_of(v + 2)] = (slopes * gate_tan * up_pre + active * up_tan).astype(BF16)

    def loss_of_tokens():
        loss_copy().wait()
        lanes = lax.broadcasted_iota(I32, (1, 128), 1)

        for i in range(32):
            tid = ids_ref[own_rows + i]
            line = loss[pl.ds(tid // 128, 1), :]
            value = jnp.sum(jnp.where(lanes == tid % 128, line, 0.0), axis=1, keepdims=True)
            scale[i : i + 1, :] = jnp.broadcast_to(value, (1, 128))

    def token_spread(t):
        @pl.when(t == 3)
        def _():
            tok_spread.third(NF)

    def token_steps(t):
        @pl.when(t == 5)
        def _():
            down_copy().start()

        @pl.when(t == 8)
        def _():
            loss_of_tokens()

        @pl.when(t == NJ)
        def _():
            down_copy().wait()

    def gather_out(g):
        @pl.when(g == 0)
        def _():
            add_out(0, 2, 0, 2, True)

        @pl.when((g == 1) | (g == 2))
        def _():
            add_out(0, GU * g, GU * g - 2, GU, False)

        @pl.when(g == 3)
        def _():
            add_out(0, GU * 3, GU * 3 - 2, 3, False)
            add_out(1, GU * 3 + 3, 0, 1, True)

        @pl.when(g > 3)
        def _():
            add_out(1, GU * g, GU * g - 2 - NJ, GU, False)

    def gather_last(g):
        @pl.when(g == 3)
        def _():
            add_last(0, 1, True, pl.ds(0, KD))

        @pl.when((g > 3) & (g < NG - 1))
        def _():
            add_last(GU * g - 2 - NJ, GU, False, pl.ds(0, KD))

    def slices(first, j, units):
        width = units * CW
        return pl.ds(pl.multiple_of(first * CW, CW), width), pl.ds(pl.multiple_of(j * CW, CW), width)

    def add_out(h, first, j, units, opens):
        at, unit = slices(first, j, units)
        part = dot(hid[:, :, at].reshape(2 * HALF, units * CW), wd[unit, :])
        acc[h] = part if opens else acc[h] + part

    def add_last(j, units, opens, cols):
        part = 0.0
        for q, weight in enumerate((wg, wu)):
            at, unit = slices(j + 2, j, units)
            later, _ = slices(j + 2 + NJ, j, units)
            left = jnp.concatenate([back[q, :, at], back[q, :, later]], axis=0)
            part = part + dot_t(left, weight[cols, unit])
        last[:, cols] = part if opens else last[:, cols] + part

    def out_term(e):
        h, n = e // 2, e % 2

        def term(block, i):
            at = (2 * n + i // 2) * CW
            return acc[h, pl.ds(pl.multiple_of(i % 2 * HALF + block, 32), 32), at : at + CW]

        return term

    def cotangents(e):
        h, n = e // 2, e % 2
        sums = row_ring.finish(e)
        weight = scale[h * 16 : (h + 1) * 16, :1]
        rows = pl.ds(stream_rows, 16)
        for i in range(2):
            cols = cols_of(2 * n + i)
            tan = weight * (lhs[0, h, rows, cols].astype(F32) + sums[2 * i + 1])
            own_tan[h * 16 : (h + 1) * 16, cols] = tan
            cot[h, 0, rows, cols] = (weight * (lhs[1, h, rows, cols].astype(F32) + sums[2 * i])).astype(BF16)
            cot[h, 1, rows, cols] = tan.astype(BF16)
        cot_spread.first(e)

    row_works = dict(
        S=lambda e: row_ring.scatter(e, out_term(e)),
        R=row_ring.relay,
        F=cotangents,
        T=cot_spread.third,
        L=cot_spread.last,
    )

    def in_order(works, names):
        for name in names.split():
            works[name[0]](int(name[1]))

    def at_steps(works, table):
        def steps(t):
            for step, names in table:

                @pl.when(t == step)
                def _():
                    in_order(works, names)

        return steps

    done = NJ - 4 + LAG[8]
    sweep(
        0, NJ, NJ - NG, multiply_in, pre_rings, hid_spread, shares_in, gather_out, token_steps,
        (token_spread, at_steps(row_works, ((done, "S0 S1"), (done + 2, "R0 R1"), (done + 3, "S2 S3")))),
    )
    in_order(row_works, "F0 F1 R2 R3 T0 T1 F2 L0 F3 L1")

    def multiply_back(k):
        @pl.when(k == NJ + 3)
        def _():
            cot_spread.last(2)
            cot_spread.last(3)

        sl = lax.rem(k, NS)
        for i in range(GU):
            v = jnp.maximum(GU * (k - NJ) - 2 + i, 0)
            left = cot[v // NJ].reshape(TOK, KD)
            both = dot_t(left, wd[pl.ds(pl.multiple_of(v % NJ * CW, CW), CW), :])
            res[sl, 2 * i] = both[:HALF]
            res[sl, 2 * i + 1] = both[HALF:]

    def shares_back(k, sums, skip):
        for i in range(skip, GU):
            v = GU * (k - NJ) - 2 + i
            backward, back_tan = sums[2 * (i - skip)], sums[2 * (i - skip) + 1]

            @pl.when(v >= 0)
            def _():
                active, slopes, curves = silu_parts(pre[2 * NJ + v, 0])
                up_pre, gate_tan, up_tan = pre[2 * NJ + v, 1], pre[v, 0], pre[v, 1]
                gate_back = (
                    back_tan * up_pre * slopes
                    + backward * up_tan * slopes
                    + backward * up_pre * curves * gate_tan
                )
                up_back = back_tan * active + backward * slopes * gate_tan
                back[0, share_rows, cols_of(v + 2)] = gate_back.astype(BF16)
                back[1, share_rows, cols_of(v + 2)] = up_back.astype(BF16)

    def last_term(f):
        h, n = f // 2, f % 2

        def term(block, i):
            at = (2 * n + i) * CW
            return last[pl.ds(pl.multiple_of(h * HALF + block, 32), 32), at : at + CW]

        return term

    def finish_last(f):
        h, n = f // 2, f % 2
        sums = last_ring.finish(f)
        for i in range(2):
            at = (2 * n + i) * CW
            rows = slice(h * 16, (h + 1) * 16)
            out_ref[rows, at : at + CW] = own_tan[rows, at : at + CW] + sums[i]

    last_works = dict(
        S=lambda f: last_ring.scatter(f, last_term(f)),
        R=last_ring.relay,
        F=finish_last,
    )

    sweep(
        NJ, NJ + NG, NJ - NG, multiply_back, back_rings, back_spread, shares_back, gather_last,
        None, (at_steps(row_works, ((NJ + 1, "T2"), (NJ + 2, "T3"))),), 1,
    )
    for n in range(2):
        add_last(GU * (NG - 1) - 2 - NJ, GU, False, pl.ds(n * KD // 2, KD // 2))
        in_order(last_works, f"S{n} S{n + 2}")
    in_order(last_works, "R0 R2 R1 R3 F0 F2 F1 F3")


def ring_buffers(arrays, rows, width, dtype, x_dtype):
    half = rows // 2
    shapes = ((arrays, rows), (arrays, rows), (2, arrays, rows), (2, arrays, rows))
    return [pltpu.VMEM((NS, *shape, width), dtype) for shape in shapes] + [
        pltpu.VMEM((NS, arrays, half, width), x_dtype) for _ in range(2)
    ]


def short_buffers(arrays, rows, width):
    half = rows // 2
    shapes = ((arrays, rows), (arrays, rows), (2, arrays, rows), (2, 2, arrays, half), (arrays, half), (arrays, half))
    return [pltpu.VMEM((NS, *shape, width), BF16) for shape in shapes]


def block(tokens, words, token_ids, loss_weight, gate_weight, up_weight, down_weight):
    vmem = lambda shape, dtype: pltpu.VMEM(shape, dtype)
    sem = lambda *shape: pltpu.SemaphoreType.DMA(shape)
    anywhere = pl.BlockSpec(memory_space=pl.ANY)
    inside = pl.BlockSpec(memory_space=pltpu.VMEM)
    scalars = pl.BlockSpec(memory_space=pltpu.SMEM)
    return pl.pallas_call(
        block_kernel,
        out_shape=jax.ShapeDtypeStruct((32, KD), F32),
        in_specs=[inside, inside, scalars, anywhere, anywhere, anywhere, anywhere],
        out_specs=inside,
        scratch_shapes=[
            vmem((2, KD, HW), BF16),
            vmem((HW, KD), BF16),
            vmem(loss_weight.shape, F32),
            vmem((32, 128), F32),
            vmem((2, 2, HALF, KD), BF16),
            vmem((2, 2, HALF, KD), BF16),
            vmem((2, HALF, WIN), BF16),
            vmem((2, HALF, WIN), BF16),
            vmem((NS, 8, HALF, CW), F32),
            vmem((NS, 8, HALF // 2, CW), F32),
            vmem((NK, 16, 16, CW), F32),
            *ring_buffers(8, 16, CW, I16, I16),
            *ring_buffers(8, 16, CW, BF16, BF16),
            vmem((4 * NJ, 2, 8, CW), F32),
            vmem((NS, 8, 32, CW), F32),
            *short_buffers(4, 32, CW),
            vmem((NS, 4, 32, CW), F32),
            *short_buffers(2, 32, CW),
            vmem((2, TOK, KD), F32),
            vmem((TOK, KD), F32),
            vmem((32, KD), F32),
            sem(1, NJ + 2),
            sem(NS),
            sem(NS),
            sem(NS, 4),
            sem(NS, 4),
            sem(NS, 5),
            sem(NS, 5),
            sem(NS, 4),
            sem(NS, 4),
            sem(NF + 1, 2),
            sem(NF + 1, 6),
        ],
        compiler_params=pltpu.CompilerParams(
            collective_id=0, has_side_effects=True, vmem_limit_bytes=67043328
        ),
    )(tokens, words, token_ids, loss_weight, gate_weight, up_weight, down_weight)


def on_device(tokens, probe_words, token_ids, loss_weight, gate_weight, up_weight, down_weight):
    return block(
        tokens, probe_words.T, token_ids, loss_weight.reshape(-1, 128), gate_weight, up_weight, down_weight
    )


def solution(mesh):
    return jax.shard_map(
        on_device,
        mesh=mesh,
        in_specs=(
            P("row", "col"),
            P(None, "col"),
            P(),
            P(),
            P("col", "row"),
            P("col", "row"),
            P("row", "col"),
        ),
        out_specs=P("row", "col"),
        check_vma=False,
    )
```
